32 devices in a mesh: slab: 16 (over z, x, core), chan: 2 (over y).
Axes of the slice: x: 2, y: 2, z: 4, core: 2. Of those that a mesh axis runs over, the one named last changes fastest.
Arguments:
- species: int32 [4096], P('slab'), may hold values from 0 to 4
- atom_count: int32 [16], P('slab'), may hold values from 192 to 256, as said below
- halo_index: int32 [16, 2, 128], P('slab'), may hold values from 0 to 255, as said below
- edge_count: int32 [16, 2], P('slab'), may hold values from 512 to 12288, as said below
- inner_edges: int32 [2, 196608], P(None, 'slab'), may hold values from 0 to 255, as said below
- outer_edges: int32 [2, 65536], P(None, 'slab'), may hold values from 0 to 255, as said below
- inner_vec: float32 [3, 196608], P(None, 'slab'), may hold values from -4.8 to 4.8, as said below
- outer_vec: float32 [3, 65536], P(None, 'slab'), may hold values from -4.8 to 4.8, as said below
- embed_table: bfloat16 [64, 5], replicated, may hold values from -6 to 6
- radial_in: bfloat16 [2, 64, 8], replicated, may hold values from -2 to 2
- radial_mid: bfloat16 [2, 64, 64], replicated, may hold values from -0.75 to 0.75
- radial_out: bfloat16 [2, 10, 64, 64], P(None, None, 'chan'), may hold values from -0.75 to 0.75
- mix_in: bfloat16 [2, 3, 64, 64], P(None, None, 'chan'), may hold values from -0.75 to 0.75
- mix_scalar: bfloat16 [2, 192, 64], replicated, may hold values from -0.75 to 0.75
- mix_irrep: bfloat16 [2, 2, 64, 64], replicated, may hold values from -0.75 to 0.75
- readout: float32 [64], replicated, may hold values from -0.75 to 0.75
- species_energy: float32 [5], replicated, may hold values from -6 to -2
Outputs:
- node_state: float32 [9, 64, 4096], P(None, None, 'slab')
- atom_energy: float32 [4096], P('slab')
- mean_energy: float32 [], replicated
The draws below stay inside these ranges and needn't reach their ends.
Inputs may be any that keep to these rules, and one draw needn't show every extreme that they name: `atom_count`: each slab holds between 192 and 256 live atoms (rounded down), live slots first; some slab holds exactly 256. `halo_index`: every entry names a live atom of its own slab. `edge_count`: column 0 lies between 1536 and 12288, column 1 between 512 and 4096 (rounded down); live slots come first in each list; each column reaches its most in some slab. `inner_edges`: both rows name live atoms of the same slab, in every slot. `outer_edges`: row 0 lies below 256; row 1 names a live atom of the slab, in every slot. `inner_vec`: every displacement is shorter than 4.8; nearly all are 0.9 or longer, and a rare few are shorter. `outer_vec`: every displacement is shorter than 4.8; nearly all are 0.9 or longer, and a rare few are shorter.
All inputs are finite; a program needn't handle non-finite values.
Results may differ from the reference program's by a relative error of at most 0.00045.
Values may be sent and summed in bfloat16 or wider, within the bound.
A program may use at most 64 MiB of HBM per device.

```python
import math
import jax
import jax.numpy as jnp
import numpy as np
from jax import lax

C = 64
NB = 8
RH = 64
NPATH = 10
NSPEC = 5
LAYERS = 2
A_DEV = 256
H_DEV = 128
E_IN = 12288
E_OUT = 4096
ATOMS = 4096


def slab_atoms(key):
    base_key = jax.random.fold_in(key, 11)
    slab_total = ATOMS // A_DEV
    counts = jax.random.randint(base_key, (slab_total,), 3 * A_DEV // 4, A_DEV + 1)
    fullest = jax.random.randint(jax.random.fold_in(base_key, 1), (), 0, slab_total)
    return jnp.where(jnp.arange(slab_total) == fullest, A_DEV, counts).astype(jnp.int32)


def live_edges(key, salt, slots):
    base_key = jax.random.fold_in(key, salt)
    slab_total = ATOMS // A_DEV
    counts = jax.random.randint(base_key, (slab_total,), slots // 8, slots + 1)
    fullest = jax.random.randint(jax.random.fold_in(base_key, 1), (), 0, slab_total)
    return jnp.where(jnp.arange(slab_total) == fullest, slots, counts).astype(jnp.int32)


def displacement(key, salt, slots):
    base_key = jax.random.fold_in(key, salt)
    total = slots * (ATOMS // A_DEV)
    heading = jax.random.normal(jax.random.fold_in(base_key, 1), (3, total), jnp.float32)
    radius = jax.random.uniform(jax.random.fold_in(base_key, 2), (total,), jnp.float32, 0.9, 4.8)
    scale = radius / jnp.sqrt(jnp.sum(heading * heading, axis=0) + 0.001)
    return heading * scale[None, :]


def draw_atom_count(key, part):
    return slab_atoms(key)


def draw_halo_index(key, part):
    counts = slab_atoms(key)
    slab_total = ATOMS // A_DEV
    return jax.random.randint(jax.random.fold_in(key, 21), (slab_total, 2, H_DEV), 0, counts[:, None, None]).astype(jnp.int32)


def draw_edge_count(key, part):
    return jnp.stack([live_edges(key, 31, E_IN), live_edges(key, 41, E_OUT)], axis=1)


def draw_inner_edges(key, part):
    counts = slab_atoms(key)
    slab_total = ATOMS // A_DEV
    repeated = jnp.repeat(counts, E_IN, total_repeat_length=slab_total * E_IN)
    return jax.random.randint(jax.random.fold_in(key, 51), (2, slab_total * E_IN), 0, repeated[None, :]).astype(jnp.int32)


def draw_outer_edges(key, part):
    counts = slab_atoms(key)
    slab_total = ATOMS // A_DEV
    repeated = jnp.repeat(counts, E_OUT, total_repeat_length=slab_total * E_OUT)
    halo_slot = jax.random.randint(jax.random.fold_in(key, 61), (slab_total * E_OUT,), 0, 2 * H_DEV)
    targets = jax.random.randint(jax.random.fold_in(key, 62), (slab_total * E_OUT,), 0, repeated)
    return jnp.stack([halo_slot, targets], axis=0).astype(jnp.int32)


def draw_inner_vec(key, part):
    return displacement(key, 71, E_IN)


def draw_outer_vec(key, part):
    return displacement(key, 81, E_OUT)


def with_ends(entries, key, least, largest):
    longest = entries.shape.index(max(entries.shape))
    spots = []
    for shift in (0, 1):
        where = [jax.random.randint(jax.random.fold_in(key, axis), (), 0, length) for axis, length in enumerate(entries.shape)]
        where[longest] = (where[longest] + shift) % entries.shape[longest]
        spots.append(tuple(where))
    return entries.at[spots[0]].set(least).at[spots[1]].set(largest)


def block_scale(key, extent, cuts, low, largest):
    def one(dim, shards_of):
        draws = jax.random.uniform(jax.random.fold_in(jax.random.fold_in(key, 6), dim), (shards_of,), jnp.float32, low / len(cuts), largest / len(cuts))
        return jnp.repeat(jnp.exp(draws), extent[dim] // shards_of).reshape((-1,) + (1,) * (len(extent) - dim - 1))

    level = one(*cuts[0])
    for cut in cuts[1:]:
        level = level * one(*cut)
    return level


def rank_bounds(amount, lean):
    weights = [(1 << 20) // math.isqrt(grade ** lean) + 1 for grade in range(1, amount + 1)]
    width = 1 + sum(weights) // (1 << 30)
    return np.cumsum(np.array([max(1, weight // width) for weight in weights]))


def ranked_ids(own_key, extent, count, skew):
    listing = rank_bounds(count, skew)
    pick = jax.random.randint(jax.random.fold_in(own_key, 1), extent, 0, int(listing[count - 1]))
    grade = jnp.searchsorted(jnp.asarray(listing, jnp.int32), pick, side="right")
    return jax.random.permutation(jax.random.fold_in(own_key, 2), count)[grade].astype(jnp.int32)


def centred(rng, extent, width, reach, cuts=(), kind=jnp.bfloat16):
    gain = block_scale(rng, extent, cuts, -0.22, 0.18) if cuts else 1.0
    values = jax.random.normal(rng, extent, jnp.float32) * width * gain
    return jnp.minimum(jnp.maximum(values, -reach), reach).astype(kind)


def setup_inputs(seed: int = 0) -> dict:
    seeds = jax.random.split(jax.random.key(seed), 18)
    return {
        "species": with_ends(ranked_ids(seeds[0], (ATOMS,), NSPEC, 2), jax.random.fold_in(seeds[0], 3), 0, NSPEC - 1).astype(jnp.int32),
        "atom_count": draw_atom_count(jax.random.fold_in(seeds[17], 71), 0),
        "halo_index": draw_halo_index(jax.random.fold_in(seeds[17], 71), 0),
        "edge_count": draw_edge_count(jax.random.fold_in(seeds[17], 71), 0),
        "inner_edges": draw_inner_edges(jax.random.fold_in(seeds[17], 71), 0),
        "outer_edges": draw_outer_edges(jax.random.fold_in(seeds[17], 71), 0),
        "inner_vec": draw_inner_vec(jax.random.fold_in(seeds[17], 71), 0),
        "outer_vec": draw_outer_vec(jax.random.fold_in(seeds[17], 71), 0),
        "embed_table": centred(seeds[8], (C, NSPEC), 1.0, 6.0),
        "radial_in": centred(seeds[9], (LAYERS, RH, NB), NB ** -0.5, 2.0),
        "radial_mid": centred(seeds[10], (LAYERS, RH, RH), RH ** -0.5, 0.75),
        "radial_out": centred(seeds[11], (LAYERS, NPATH, C, RH), RH ** -0.5, 0.75, ((2, 2),)),
        "mix_in": centred(seeds[12], (LAYERS, 3, C, C), C ** -0.5, 0.75, ((2, 2),)),
        "mix_scalar": centred(seeds[13], (LAYERS, 3 * C, C), C ** -0.5, 0.75),
        "mix_irrep": centred(seeds[14], (LAYERS, 2, C, C), C ** -0.5, 0.75),
        "readout": centred(seeds[15], (C,), C ** -0.5, 0.75, (), jnp.float32),
        "species_energy": jnp.clip(jax.random.uniform(seeds[16], (NSPEC,), jnp.float32, -6.0, -2.0), -6.0, -2.0),
    }


cutoff = 5.0
neighbour_norm = 1.0 / math.sqrt(48.0)
root_three = math.sqrt(3.0)
half_root = 0.5 * math.sqrt(3.0)

def geometry(vectors, basis_total):
    squared = lax.optimization_barrier(jnp.sum(vectors * vectors, axis=0))
    length = jnp.sqrt(squared)
    softened = jnp.sqrt(squared + 0.25)
    directions = vectors / softened[None, :]
    fraction = jnp.minimum(length / cutoff, 1.0)
    envelope = 1.0 - 28.0 * fraction ** 6 + 48.0 * fraction ** 7 - 21.0 * fraction ** 8
    orders = jnp.arange(1, basis_total + 1, dtype=jnp.float32)[:, None]
    bessel = math.sqrt(2.0 / cutoff) * jnp.sin(orders * (math.pi / cutoff) * length[None, :]) / softened[None, :] * envelope[None, :]
    return (directions, bessel)

def edge_messages(source, directions, bessel, live_mask, layer_weights):
    first_layer, middle_layer, last_layer = layer_weights
    hidden = jax.nn.silu(jnp.dot(first_layer, bessel.astype(jnp.bfloat16), preferred_element_type=jnp.float32)).astype(jnp.bfloat16)
    hidden = jax.nn.silu(jnp.dot(middle_layer, hidden, preferred_element_type=jnp.float32)).astype(jnp.bfloat16)
    path_total, channels, breadth = last_layer.shape
    weights = jnp.dot(last_layer.reshape(path_total * channels, breadth), hidden, preferred_element_type=jnp.float32)
    weights = weights.reshape(path_total, channels, hidden.shape[1])
    features = source.astype(jnp.float32)
    scalar_in = features[0]
    vector_in = [features[1], features[2], features[3]]
    tensor_in = [features[4], features[5], features[6], features[7], features[8]]
    unit_parts = [directions[0][None, :], directions[1][None, :], directions[2][None, :]]
    unit_square = unit_parts[0] * unit_parts[0] + unit_parts[1] * unit_parts[1] + unit_parts[2] * unit_parts[2]
    harmonic = [root_three * unit_parts[0] * unit_parts[1], root_three * unit_parts[1] * unit_parts[2], 0.5 * (3.0 * unit_parts[2] * unit_parts[2] - unit_square), root_three * unit_parts[0] * unit_parts[2], half_root * (unit_parts[0] * unit_parts[0] - unit_parts[1] * unit_parts[1])]
    vector_along = vector_in[0] * unit_parts[0] + vector_in[1] * unit_parts[1] + vector_in[2] * unit_parts[2]
    tensor_along = tensor_in[0] * harmonic[0] + tensor_in[1] * harmonic[1] + tensor_in[2] * harmonic[2] + tensor_in[3] * harmonic[3] + tensor_in[4] * harmonic[4]
    out_scalar = weights[0] * scalar_in + weights[1] * tensor_along + weights[2] * vector_along
    cross_term = [vector_in[1] * unit_parts[2] - vector_in[2] * unit_parts[1], vector_in[2] * unit_parts[0] - vector_in[0] * unit_parts[2], vector_in[0] * unit_parts[1] - vector_in[1] * unit_parts[0]]
    gradient = [0.5 * (root_three * tensor_in[0] * unit_parts[1] - tensor_in[2] * unit_parts[0] + root_three * tensor_in[3] * unit_parts[2] + root_three * tensor_in[4] * unit_parts[0]), 0.5 * (root_three * tensor_in[0] * unit_parts[0] + root_three * tensor_in[1] * unit_parts[2] - tensor_in[2] * unit_parts[1] - root_three * tensor_in[4] * unit_parts[1]), 0.5 * (root_three * tensor_in[1] * unit_parts[1] + 2.0 * tensor_in[2] * unit_parts[2] + root_three * tensor_in[3] * unit_parts[0])]
    out_vector = [weights[3] * scalar_in * unit_parts[0] + weights[4] * vector_in[0] + weights[5] * cross_term[0] + weights[6] * gradient[0], weights[3] * scalar_in * unit_parts[1] + weights[4] * vector_in[1] + weights[5] * cross_term[1] + weights[6] * gradient[1], weights[3] * scalar_in * unit_parts[2] + weights[4] * vector_in[2] + weights[5] * cross_term[2] + weights[6] * gradient[2]]
    symmetric = [half_root * (vector_in[0] * unit_parts[1] + vector_in[1] * unit_parts[0]), half_root * (vector_in[1] * unit_parts[2] + vector_in[2] * unit_parts[1]), 0.5 * (3.0 * vector_in[2] * unit_parts[2] - vector_along), half_root * (vector_in[0] * unit_parts[2] + vector_in[2] * unit_parts[0]), half_root * (vector_in[0] * unit_parts[0] - vector_in[1] * unit_parts[1])]
    out_tensor = [weights[7] * scalar_in * harmonic[0] + weights[8] * tensor_in[0] + weights[9] * symmetric[0], weights[7] * scalar_in * harmonic[1] + weights[8] * tensor_in[1] + weights[9] * symmetric[1], weights[7] * scalar_in * harmonic[2] + weights[8] * tensor_in[2] + weights[9] * symmetric[2], weights[7] * scalar_in * harmonic[3] + weights[8] * tensor_in[3] + weights[9] * symmetric[3], weights[7] * scalar_in * harmonic[4] + weights[8] * tensor_in[4] + weights[9] * symmetric[4]]
    stacked = jnp.stack([out_scalar] + out_vector + out_tensor)
    return stacked * live_mask[None, None, :]

def mix_channels(weights, rounded):
    scalar_part = jnp.dot(weights[0], rounded[0], preferred_element_type=jnp.float32)[None]
    vector_part = jnp.einsum('oi,kia->koa', weights[1].astype(jnp.float32), rounded[1:4].astype(jnp.float32))
    tensor_part = jnp.einsum('oi,kia->koa', weights[2].astype(jnp.float32), rounded[4:9].astype(jnp.float32))
    return jnp.concatenate([scalar_part, vector_part, tensor_part], axis=0)

def gate_update(aggregated, scalar_weight, irrep_weight):
    channels = aggregated.shape[1]
    mixed_scalar = jnp.dot(scalar_weight, aggregated[0], preferred_element_type=jnp.float32)
    mixed_vector = jnp.einsum('oi,kia->koa', irrep_weight[0].astype(jnp.float32), aggregated[1:4].astype(jnp.float32))
    mixed_tensor = jnp.einsum('oi,kia->koa', irrep_weight[1].astype(jnp.float32), aggregated[4:9].astype(jnp.float32))
    new_scalar = jax.nn.silu(mixed_scalar[:channels])[None]
    new_vector = jax.nn.sigmoid(mixed_scalar[channels:2 * channels])[None] * mixed_vector
    new_tensor = jax.nn.sigmoid(mixed_scalar[2 * channels:])[None] * mixed_tensor
    return jnp.concatenate([new_scalar, new_vector, new_tensor], axis=0)

def reference(species, atom_count, halo_index, edge_count, inner_edges, outer_edges, inner_vec, outer_vec, embed_table, radial_in, radial_mid, radial_out, mix_in, mix_scalar, mix_irrep, readout, species_energy):
    slab_total = ATOMS // A_DEV
    onehot = species[None, :] == jnp.arange(NSPEC, dtype=jnp.int32)[:, None]
    scalar_init = jnp.dot(embed_table, onehot.astype(jnp.bfloat16), preferred_element_type=jnp.float32)
    node_state = jnp.concatenate([scalar_init[None], jnp.zeros((8, C, ATOMS), jnp.float32)], axis=0)
    offsets = (jnp.arange(slab_total, dtype=jnp.int32) * A_DEV)[:, None]
    inner_source = inner_edges[0].reshape(slab_total, E_IN) + offsets
    inner_target = inner_edges[1].reshape(slab_total, E_IN)
    halo_before = jnp.roll(halo_index, 1, axis=0)[:, 1, :] + jnp.roll(offsets, 1, axis=0)
    halo_after = jnp.roll(halo_index, -1, axis=0)[:, 0, :] + jnp.roll(offsets, -1, axis=0)
    halo_atoms = jnp.concatenate([halo_before, halo_after], axis=1)
    halo_slot = outer_edges[0].reshape(slab_total, E_OUT)
    outer_source = jnp.take_along_axis(halo_atoms, halo_slot, axis=1)
    outer_target = outer_edges[1].reshape(slab_total, E_OUT)
    sources = jnp.concatenate([inner_source, outer_source], axis=1).astype(jnp.int32)
    targets = jnp.concatenate([inner_target, outer_target], axis=1).astype(jnp.int32)
    vectors = jnp.concatenate([inner_vec.reshape(3, slab_total, E_IN), outer_vec.reshape(3, slab_total, E_OUT)], axis=2)
    vectors = jnp.transpose(vectors, (1, 0, 2))
    inner_live = (jnp.arange(E_IN, dtype=jnp.int32)[None, :] < edge_count[:, 0:1]).astype(jnp.float32)
    outer_live = (jnp.arange(E_OUT, dtype=jnp.int32)[None, :] < edge_count[:, 1:2]).astype(jnp.float32)
    live_mask = jnp.concatenate([inner_live, outer_live], axis=1)
    for layer_index in range(LAYERS):
        rounded = node_state.astype(jnp.bfloat16)
        features = mix_channels(mix_in[layer_index], rounded).astype(jnp.bfloat16)
        layer_weights = (radial_in[layer_index], radial_mid[layer_index], radial_out[layer_index])

        def per_slab(carried, pieces):
            slab_sources, slab_targets, slab_vectors, slab_live = pieces
            source = jnp.take(features, slab_sources, axis=2)
            directions, bessel = geometry(slab_vectors, NB)
            message = edge_messages(source, directions, bessel, slab_live, layer_weights)
            summed = jnp.zeros((9, C, A_DEV), jnp.float32).at[:, :, slab_targets].add(message)
            return (carried, summed)
        _, slab_sums = lax.scan(per_slab, jnp.zeros((), jnp.float32), (sources, targets, vectors, live_mask))
        aggregated = jnp.transpose(slab_sums, (1, 2, 0, 3)).reshape(9, C, ATOMS)
        aggregated = (aggregated * neighbour_norm).astype(jnp.bfloat16)
        node_state = node_state + gate_update(aggregated, mix_scalar[layer_index], mix_irrep[layer_index])
    readout_part = lax.optimization_barrier(jnp.sum(node_state[0] * readout[:, None], axis=0))
    species_part = lax.optimization_barrier(jnp.sum(onehot.astype(jnp.float32) * species_energy[:, None], axis=0))
    live_atoms = (jnp.arange(ATOMS, dtype=jnp.int32) % A_DEV < jnp.repeat(atom_count, A_DEV)).astype(jnp.float32)
    atom_energy = (readout_part + species_part) * live_atoms
    mean_energy = jnp.sum(atom_energy) / ATOMS
    return (node_state, atom_energy, mean_energy)
```

```python
import functools
import math

import jax
import jax.numpy as jnp
from jax import lax
from jax.experimental import pallas as pl
from jax.experimental.pallas import tpu as pltpu
from jax.sharding import PartitionSpec as P

cutoff = 5.0
neighbour_norm = 1.0 / math.sqrt(48.0)
root_three = math.sqrt(3.0)
half_root = 0.5 * math.sqrt(3.0)
f32 = jnp.float32
bf16 = jnp.bfloat16


def dot(a, b):
    return jnp.dot(a, b, preferred_element_type=f32)


def dot_nt(a, b):
    return lax.dot_general(a, b, (((1,), (1,)), ((), ())), preferred_element_type=f32)


def sigmoid(v):
    return 0.5 * jnp.tanh(0.5 * v) + 0.5


def silu(v):
    half = 0.5 * v
    return half * jnp.tanh(half) + half


def onehot_rows(index, rows):
    slots = lax.broadcasted_iota(jnp.int32, (rows, index.shape[1]), 0)
    return jnp.where(slots == index, 1.0, 0.0).astype(bf16)


def unit(vec):
    x, y, z = vec[0:1], vec[1:2], vec[2:3]
    squared = x * x + y * y + z * z
    inverse = lax.rsqrt(squared + 0.25)
    return squared, inverse, x * inverse, y * inverse, z * inverse


def bessel_rows(squared, inverse, orders):
    length = jnp.sqrt(squared)
    fraction = jnp.minimum(length * (1.0 / cutoff), 1.0)
    cube = fraction * fraction * fraction
    sixth = cube * cube
    envelope = 1.0 - sixth * (28.0 - fraction * (48.0 - 21.0 * fraction))
    half = length * (0.5 * math.pi / cutoff)
    h2 = half * half
    sine = 1.0
    cosine = 1.0
    for order in range(12, 0, -2):
        sine = 1.0 - sine * h2 * (1.0 / ((order + 1) * order))
        cosine = 1.0 - cosine * h2 * (1.0 / (order * (order - 1)))
    sine = sine * half
    twice_cos = 2.0 - 4.0 * sine * sine
    first = 2.0 * sine * cosine
    scale = math.sqrt(2.0 / cutoff) * inverse * envelope
    before, now = jnp.zeros_like(first), first * scale
    rows = []
    for _ in range(orders):
        rows.append(now)
        before, now = now, twice_cos * now - before
    return jnp.concatenate(rows, axis=0)


def harmonics(x, y, z):
    return [
        root_three * x * y,
        root_three * y * z,
        0.5 * (2.0 * z * z - x * x - y * y),
        root_three * x * z,
        half_root * (x * x - y * y),
    ]


def first_kernel(
    block,
    count_ref,
    species_ref,
    halo_species_ref,
    inner_edges_ref,
    outer_edges_ref,
    inner_vec_ref,
    outer_vec_ref,
    embed_ref,
    mix_ref,
    radial_in_ref,
    radial_mid_ref,
    radial_out_ref,
    agg_ref,
    inner_hidden_ref,
    outer_hidden_ref,
    acc_ref,
    table_ref,
    mess_ref,
):
    breadth = radial_out_ref.shape[1]
    chans = mix_ref.shape[0]
    atoms = species_ref.shape[1]
    kinds = embed_ref.shape[1]
    for slot, ref in enumerate((species_ref, halo_species_ref)):
        init = dot(embed_ref[...], onehot_rows(ref[...], kinds)).astype(bf16)
        table_ref[slot] = dot(mix_ref[...], init).astype(bf16)
    acc_ref[...] = jnp.zeros_like(acc_ref)

    def visit(slot, edges_ref, vec_ref, hidden_ref, live, step):
        offset = pl.multiple_of(step * block, block)
        span = pl.ds(offset, block)
        source = onehot_rows(edges_ref[0:1, span], table_ref.shape[2])
        gathered = dot(table_ref[slot], source)
        squared, inverse, x, y, z = unit(vec_ref[:, span])
        basis = bessel_rows(squared, inverse, radial_in_ref.shape[1]).astype(bf16)
        hidden = silu(dot(radial_in_ref[...], basis)).astype(bf16)
        hidden = silu(dot(radial_mid_ref[...], hidden)).astype(bf16)
        hidden_ref[:, span] = hidden[breadth:]
        weights = dot(radial_out_ref[...], hidden[:breadth])
        q = harmonics(x, y, z)
        lanes = lax.broadcasted_iota(jnp.int32, (1, block), 1) + offset
        target = jnp.where(lanes < live, edges_ref[1:2, span], -1)
        by_vector = weights[chans : 2 * chans] * gathered
        by_tensor = weights[2 * chans : 3 * chans] * gathered
        mess_ref[0:chans] = (weights[0:chans] * gathered).astype(bf16)
        for k, part in enumerate((x, y, z)):
            mess_ref[(1 + k) * chans : (2 + k) * chans] = (by_vector * part).astype(bf16)
        for k, part in enumerate(q):
            mess_ref[(4 + k) * chans : (5 + k) * chans] = (by_tensor * part).astype(bf16)
        acc_ref[...] += dot_nt(mess_ref[...], onehot_rows(target, atoms))

    def run(slot, edges_ref, vec_ref, hidden_ref, live):
        def body(step, carry):
            visit(slot, edges_ref, vec_ref, hidden_ref, live, step)
            return carry

        lax.fori_loop(0, lax.div(live + (block - 1), block), body, 0)

    run(0, inner_edges_ref, inner_vec_ref, inner_hidden_ref, count_ref[0, 0])
    run(1, outer_edges_ref, outer_vec_ref, outer_hidden_ref, count_ref[0, 1])
    agg_ref[...] = (acc_ref[...] * neighbour_norm).astype(bf16)


def second_kernel(
    block,
    finish,
    count_ref,
    table_ref,
    edges_ref,
    vec_ref,
    hidden_ref,
    radial_out_ref,
    start_ref,
    out_ref,
    acc_ref,
    weight_ref,
    source_ref,
    mess_ref,
):
    chans = table_ref.shape[0] // 9
    atoms = out_ref.shape[1]
    if start_ref is None:
        acc_ref[...] = jnp.zeros_like(acc_ref)
    else:
        acc_ref[...] = start_ref[...]
    live = count_ref[0, 1 if finish else 0]

    def body(step, carry):
        offset = pl.multiple_of(step * block, block)
        span = pl.ds(offset, block)
        onehot = onehot_rows(edges_ref[0:1, span], table_ref.shape[1])
        source_ref[...] = dot(table_ref[...], onehot)
        weight_ref[...] = dot(radial_out_ref[...], hidden_ref[:, span])
        _, _, x_row, y_row, z_row = unit(vec_ref[:, span])
        q_rows = harmonics(x_row, y_row, z_row)
        height, width = 16, 128
        for lane in range(0, block, width):
            cols = slice(lane, lane + width)

            def wide(row):
                return jnp.broadcast_to(row[:, cols], (height, width))

            x, y, z = wide(x_row), wide(y_row), wide(z_row)
            q = [wide(row) for row in q_rows]
            hx, hy, hz = half_root * x, half_root * y, half_root * z
            for low in range(0, chans, height):

                def at(ref, k):
                    return ref[k * chans + low : k * chans + low + height, cols]

                def put(k, value):
                    mess_ref[k * chans + low : k * chans + low + height, cols] = value.astype(bf16)

                s = at(source_ref, 0)
                v = [at(source_ref, k) for k in (1, 2, 3)]
                t = [at(source_ref, k) for k in (4, 5, 6, 7, 8)]
                along = v[0] * x + v[1] * y + v[2] * z
                tq = t[0] * q[0] + t[1] * q[1] + t[2] * q[2] + t[3] * q[3] + t[4] * q[4]
                put(0, at(weight_ref, 0) * s + at(weight_ref, 1) * tq + at(weight_ref, 2) * along)
                ws = at(weight_ref, 3) * s
                w4, w5, w6 = at(weight_ref, 4), at(weight_ref, 5), at(weight_ref, 6)
                cross = [
                    v[1] * z - v[2] * y,
                    v[2] * x - v[0] * z,
                    v[0] * y - v[1] * x,
                ]
                t3 = 0.5 * t[2]
                grad = [
                    hy * t[0] - x * t3 + hz * t[3] + hx * t[4],
                    hx * t[0] + hz * t[1] - y * t3 - hy * t[4],
                    hy * t[1] + z * t[2] + hx * t[3],
                ]
                for k, part in enumerate((x, y, z)):
                    put(1 + k, ws * part + w4 * v[k] + w5 * cross[k] + w6 * grad[k])
                ws = at(weight_ref, 7) * s
                w8, w9 = at(weight_ref, 8), at(weight_ref, 9)
                sym = [
                    hy * v[0] + hx * v[1],
                    hz * v[1] + hy * v[2],
                    1.5 * v[2] * z - 0.5 * along,
                    hz * v[0] + hx * v[2],
                    hx * v[0] - hy * v[1],
                ]
                for k in range(5):
                    put(4 + k, ws * q[k] + w8 * t[k] + w9 * sym[k])
        lanes = lax.broadcasted_iota(jnp.int32, (1, block), 1) + offset
        target = jnp.where(lanes < live, edges_ref[1:2, span], -1)
        acc_ref[...] += dot_nt(mess_ref[...], onehot_rows(target, atoms))
        return carry

    lax.fori_loop(0, lax.div(live + (block - 1), block), body, 0)
    if finish:
        out_ref[...] = (acc_ref[...] * neighbour_norm).astype(bf16)
    else:
        out_ref[...] = acc_ref[...]


def updates(agg, scalar_ref, irrep_ref, chans):
    y = dot(scalar_ref[...], agg(0))
    gate_vector = sigmoid(y[chans : 2 * chans])
    gate_tensor = sigmoid(y[2 * chans :])
    outs = [silu(y[:chans])]
    for k in range(1, 9):
        part = dot(irrep_ref[0 if k < 4 else 1], agg(k))
        outs.append((gate_vector if k < 4 else gate_tensor) * part)
    return outs


def joined(ref, chans):
    def component(k):
        return jnp.concatenate(
            [ref[i, k * chans : (k + 1) * chans] for i in range(ref.shape[0])], axis=0
        )

    return component


def middle_kernel(
    species_ref,
    halo_ref,
    agg_ref,
    embed_ref,
    mix_ref,
    scalar_ref,
    irrep_ref,
    state_ref,
    table_ref,
    send_ref,
):
    chans = embed_ref.shape[0]
    part = mix_ref.shape[1]
    outs = updates(joined(agg_ref, part), scalar_ref, irrep_ref, chans)
    outs[0] += dot(embed_ref[...], onehot_rows(species_ref[...], embed_ref.shape[1]))
    for k in range(9):
        state_ref[k] = outs[k]
        which = 0 if k == 0 else (1 if k < 4 else 2)
        table_ref[k * part : (k + 1) * part] = dot(mix_ref[which], outs[k].astype(bf16)).astype(bf16)
    for side in range(2):
        onehot = onehot_rows(halo_ref[side : side + 1], table_ref.shape[1])
        send_ref[side] = dot(table_ref[...], onehot).astype(bf16)


def last_kernel(
    species_ref,
    count_ref,
    agg_ref,
    state_in_ref,
    scalar_ref,
    irrep_ref,
    readout_ref,
    energy_ref,
    state_ref,
    atom_ref,
):
    chans = state_ref.shape[1]
    part = agg_ref.shape[1] // 9
    outs = updates(joined(agg_ref, part), scalar_ref, irrep_ref, chans)
    for k in range(9):
        outs[k] += state_in_ref[k]
        state_ref[k] = outs[k]
    atoms = state_ref.shape[2]
    total = jnp.sum(outs[0] * readout_ref[...], axis=0, keepdims=True)
    slots = lax.broadcasted_iota(jnp.int32, (energy_ref.shape[0], atoms), 0)
    total += jnp.sum(
        jnp.where(slots == species_ref[...], energy_ref[...], 0.0), axis=0, keepdims=True
    )
    lanes = lax.broadcasted_iota(jnp.int32, (1, atoms), 1)
    atom_ref[...] = jnp.where(lanes < count_ref[0], total, 0.0)


vmem = pl.BlockSpec(memory_space=pltpu.VMEM)
smem = pl.BlockSpec(memory_space=pltpu.SMEM)
params = pltpu.CompilerParams(vmem_limit_bytes=56 * 1024 * 1024)


def passed_along(array, axis, by):
    devices = lax.axis_size(axis)
    return lax.ppermute(array, axis, [(i, (i + by) % devices) for i in range(devices)])


def second_call(table, edges, vec, hidden, radial_out, count, start, block):
    rows, atoms = table.shape
    finish = start is not None
    body = functools.partial(second_kernel, block, finish)
    if not finish:
        full = body

        def body(c, t, e, v, h, r, o, *scratch):
            full(c, t, e, v, h, r, None, o, *scratch)

    operands = [count, table, edges, vec, hidden, radial_out] + ([start] if finish else [])
    return pl.pallas_call(
        body,
        out_shape=jax.ShapeDtypeStruct((rows, count_atoms(start, atoms)), bf16 if finish else f32),
        in_specs=[smem] + [vmem] * (len(operands) - 1),
        out_specs=vmem,
        scratch_shapes=[
            pltpu.VMEM((rows, count_atoms(start, atoms)), f32),
            pltpu.VMEM((radial_out.shape[0], block), f32),
            pltpu.VMEM((rows, block), f32),
            pltpu.VMEM((rows, block), bf16),
        ],
        compiler_params=params,
        cost_estimate=pl.CostEstimate(
            flops=edges.shape[1] * 1024 * 512, bytes_accessed=1 << 20, transcendentals=0
        ),
        name="outer_edges" if finish else "inner_edges",
    )(*operands)


def count_atoms(start, atoms):
    return atoms if start is None else start.shape[1]


def local(
    species,
    atom_count,
    halo_index,
    edge_count,
    inner_edges,
    outer_edges,
    inner_vec,
    outer_vec,
    embed_table,
    radial_in,
    radial_mid,
    radial_out,
    mix_in,
    mix_scalar,
    mix_irrep,
    readout,
    species_energy,
):
    atoms = species.shape[0]
    chans = embed_table.shape[0]
    part = mix_in.shape[2]
    breadth = radial_mid.shape[1]
    halo = halo_index[0]
    species_row = species[None, :]
    picked = jnp.sum(
        jnp.where(
            halo[:, :, None] == jnp.arange(atoms, dtype=jnp.int32)[None, None, :],
            species[None, None, :],
            0,
        ),
        axis=2,
    )
    halo_species = jnp.concatenate(
        [passed_along(picked[1], "slab", 1), passed_along(picked[0], "slab", -1)]
    )[None, :]
    empty = jnp.zeros((breadth, breadth), bf16)
    mid = jnp.concatenate(
        [
            jnp.concatenate([radial_mid[0], empty], axis=1),
            jnp.concatenate([empty, radial_mid[1]], axis=1),
        ],
        axis=0,
    )
    rows = 9 * part
    block = math.gcd(1024, math.gcd(inner_edges.shape[1], outer_edges.shape[1]))
    agg, inner_hidden, outer_hidden = pl.pallas_call(
        functools.partial(first_kernel, block),
        out_shape=(
            jax.ShapeDtypeStruct((rows, atoms), bf16),
            jax.ShapeDtypeStruct((breadth, inner_edges.shape[1]), bf16),
            jax.ShapeDtypeStruct((breadth, outer_edges.shape[1]), bf16),
        ),
        in_specs=[smem] + [vmem] * 11,
        out_specs=(vmem, vmem, vmem),
        scratch_shapes=[
            pltpu.VMEM((rows, atoms), f32),
            pltpu.VMEM((2, part, atoms), bf16),
            pltpu.VMEM((rows, block), bf16),
        ],
        compiler_params=params,
        name="first_layer",
    )(
        edge_count,
        species_row,
        halo_species,
        inner_edges,
        outer_edges,
        inner_vec,
        outer_vec,
        embed_table,
        mix_in[0, 0],
        radial_in.reshape(2 * breadth, -1),
        mid,
        radial_out[0][jnp.array([0, 3, 7])].reshape(3 * part, breadth),
    )
    agg_all = lax.all_gather(agg, "chan", axis=0)
    state, table, send = pl.pallas_call(
        middle_kernel,
        out_shape=(
            jax.ShapeDtypeStruct((9, chans, atoms), f32),
            jax.ShapeDtypeStruct((rows, atoms), bf16),
            jax.ShapeDtypeStruct((2, rows, halo.shape[1]), bf16),
        ),
        in_specs=[vmem] * 7,
        out_specs=(vmem, vmem, vmem),
        compiler_params=params,
        name="middle",
    )(species_row, halo, agg_all, embed_table, mix_in[1], mix_scalar[0], mix_irrep[0])
    from_left = passed_along(send[1], "slab", 1)
    from_right = passed_along(send[0], "slab", -1)
    paths = radial_out[1].reshape(-1, breadth)
    summed = second_call(table, inner_edges, inner_vec, inner_hidden, paths, edge_count, None, block)
    halo_table = jnp.concatenate([from_left, from_right], axis=1)
    agg = second_call(
        halo_table, outer_edges, outer_vec, outer_hidden, paths, edge_count, summed, block
    )
    agg_all = lax.all_gather(agg, "chan", axis=0)
    node_state, atom_energy = pl.pallas_call(
        last_kernel,
        out_shape=(
            jax.ShapeDtypeStruct((9, chans, atoms), f32),
            jax.ShapeDtypeStruct((1, atoms), f32),
        ),
        in_specs=[vmem, smem] + [vmem] * 6,
        out_specs=(vmem, vmem),
        compiler_params=params,
        name="last",
    )(
        species_row,
        atom_count,
        agg_all,
        state,
        mix_scalar[1],
        mix_irrep[1],
        readout[:, None],
        species_energy[:, None],
    )
    slabs = lax.axis_size("slab")
    energies = lax.all_gather(jnp.sum(atom_energy, axis=1), "slab", axis=0)
    mean_energy = jnp.sum(energies) / (atoms * slabs)
    return (node_state, atom_energy[0], mean_energy)


def solution(mesh):
    return jax.shard_map(
        local,
        mesh=mesh,
        in_specs=(
            P("slab"),
            P("slab"),
            P("slab", None, None),
            P("slab", None),
            P(None, "slab"),
            P(None, "slab"),
            P(None, "slab"),
            P(None, "slab"),
            P(),
            P(),
            P(),
            P(None, None, "chan", None),
            P(None, None, "chan", None),
            P(),
            P(),
            P(),
            P(),
        ),
        out_specs=(P(None, None, "slab"), P("slab"), P()),
        check_vma=False,
    )
```

```python
import functools
import math

import jax
import jax.numpy as jnp
from jax import lax
from jax.experimental import pallas as pl
from jax.experimental.pallas import tpu as pltpu
from jax.sharding import PartitionSpec as P

cutoff = 5.0
neighbour_norm = 1.0 / math.sqrt(48.0)
root_three = math.sqrt(3.0)
half_root = 0.5 * math.sqrt(3.0)
BLOCK = 1024
f32 = jnp.float32
bf16 = jnp.bfloat16


def dot(a, b):
    return jnp.dot(a, b, preferred_element_type=f32)


def dot_nt(a, b):
    return lax.dot_general(a, b, (((1,), (1,)), ((), ())), preferred_element_type=f32)


def sigmoid(v):
    return 0.5 * jnp.tanh(0.5 * v) + 0.5


def silu(v):
    half = 0.5 * v
    return half * jnp.tanh(half) + half


def onehot_rows(index, rows):
    slots = lax.broadcasted_iota(jnp.int32, (rows, index.shape[1]), 0)
    return jnp.where(slots == index, 1.0, 0.0).astype(bf16)


def turned(matrix):
    return matrix.astype(f32).T.astype(bf16)


def initial(embed_ref, species_row):
    return dot(turned(embed_ref[...]), onehot_rows(species_row, embed_ref.shape[0]))


def unit(vec):
    x, y, z = vec[0:1], vec[1:2], vec[2:3]
    squared = x * x + y * y + z * z
    inverse = lax.rsqrt(squared + 0.25)
    return squared, inverse, x * inverse, y * inverse, z * inverse


def bessel_rows(squared, inverse, orders):
    length = jnp.sqrt(squared)
    fraction = jnp.minimum(length * (1.0 / cutoff), 1.0)
    cube = fraction * fraction * fraction
    sixth = cube * cube
    envelope = 1.0 - sixth * (28.0 - fraction * (48.0 - 21.0 * fraction))
    half = length * (0.5 * math.pi / cutoff)
    h2 = half * half
    sine = 1.0
    cosine = 1.0
    for order in range(12, 0, -2):
        sine = 1.0 - sine * h2 * (1.0 / ((order + 1) * order))
        cosine = 1.0 - cosine * h2 * (1.0 / (order * (order - 1)))
    sine = sine * half
    twice_cos = 2.0 - 4.0 * sine * sine
    first = 2.0 * sine * cosine
    scale = math.sqrt(2.0 / cutoff) * inverse * envelope
    before, now = jnp.zeros_like(first), first * scale
    rows = []
    for _ in range(orders):
        rows.append(now)
        before, now = now, twice_cos * now - before
    return jnp.concatenate(rows, axis=0)


def harmonics(x, y, z):
    return [
        root_three * x * y,
        root_three * y * z,
        0.5 * (2.0 * z * z - x * x - y * y),
        root_three * x * z,
        half_root * (x * x - y * y),
    ]


def first_kernel(
    block,
    count_ref,
    species_ref,
    halo_species_ref,
    inner_edges_ref,
    outer_edges_ref,
    inner_vec_ref,
    outer_vec_ref,
    embed_ref,
    mix_ref,
    radial_in_ref,
    radial_mid_ref,
    radial_out_ref,
    agg_ref,
    inner_hidden_ref,
    outer_hidden_ref,
    acc_ref,
    table_ref,
    mess_ref,
    both_in_ref,
    both_mid_ref,
    paths_ref,
):
    breadth = radial_out_ref.shape[3]
    chans = mix_ref.shape[2]
    atoms = species_ref.shape[1]
    for slot, ref in enumerate((species_ref, halo_species_ref)):
        init = initial(embed_ref, ref[...]).astype(bf16)
        table_ref[slot] = dot(mix_ref[0, 0], init).astype(bf16)
    acc_ref[...] = jnp.zeros_like(acc_ref)
    both_mid_ref[...] = jnp.zeros_like(both_mid_ref)
    for layer in range(2):
        span = slice(layer * breadth, (layer + 1) * breadth)
        both_in_ref[span] = turned(radial_in_ref[layer])
        both_mid_ref[span, span] = radial_mid_ref[layer]
    for k, path in enumerate((0, 3, 7)):
        paths_ref[k * chans : (k + 1) * chans] = radial_out_ref[0, path]

    def visit(slot, edges_ref, vec_ref, hidden_ref, live, step):
        offset = pl.multiple_of(step * block, block)
        span = pl.ds(offset, block)
        source = onehot_rows(edges_ref[0:1, span], table_ref.shape[2])
        gathered = dot(table_ref[slot], source)
        squared, inverse, x, y, z = unit(vec_ref[:, span])
        basis = bessel_rows(squared, inverse, radial_in_ref.shape[1]).astype(bf16)
        hidden = silu(dot(both_in_ref[...], basis)).astype(bf16)
        hidden = silu(dot(both_mid_ref[...], hidden)).astype(bf16)
        hidden_ref[:, span] = hidden[breadth:]
        weights = dot(paths_ref[...], hidden[:breadth])
        q = harmonics(x, y, z)
        lanes = lax.broadcasted_iota(jnp.int32, (1, block), 1) + offset
        target = jnp.where(lanes < live, edges_ref[1:2, span], -1)
        by_vector = weights[chans : 2 * chans] * gathered
        by_tensor = weights[2 * chans : 3 * chans] * gathered
        mess_ref[0:chans] = (weights[0:chans] * gathered).astype(bf16)
        for k, part in enumerate((x, y, z)):
            mess_ref[(1 + k) * chans : (2 + k) * chans] = (by_vector * part).astype(bf16)
        for k, part in enumerate(q):
            mess_ref[(4 + k) * chans : (5 + k) * chans] = (by_tensor * part).astype(bf16)
        acc_ref[...] += dot_nt(mess_ref[...], onehot_rows(target, atoms))

    def run(slot, edges_ref, vec_ref, hidden_ref, live):
        def body(step, carry):
            visit(slot, edges_ref, vec_ref, hidden_ref, live, step)
            return carry

        lax.fori_loop(0, lax.div(live + (block - 1), block), body, 0)

    run(0, inner_edges_ref, inner_vec_ref, inner_hidden_ref, count_ref[0, 0])
    run(1, outer_edges_ref, outer_vec_ref, outer_hidden_ref, count_ref[0, 1])
    agg_ref[...] = (acc_ref[...] * neighbour_norm).astype(bf16)


def second_kernel(
    block,
    count_ref,
    table_ref,
    halo_table_ref,
    inner_edges_ref,
    outer_edges_ref,
    inner_vec_ref,
    outer_vec_ref,
    inner_hidden_ref,
    outer_hidden_ref,
    radial_out_ref,
    out_ref,
    acc_ref,
    weight_ref,
    source_ref,
    mess_ref,
):
    chans = table_ref.shape[0] // 9
    atoms = out_ref.shape[1]
    acc_ref[...] = jnp.zeros_like(acc_ref)
    paths, _, breadth = radial_out_ref.shape[1:]
    radial = radial_out_ref[1].reshape(paths * chans, breadth)

    def visit(table_ref, edges_ref, vec_ref, hidden_ref, live, step):
        offset = pl.multiple_of(step * block, block)
        span = pl.ds(offset, block)
        onehot = onehot_rows(edges_ref[0:1, span], table_ref.shape[1])
        source_ref[...] = dot(table_ref[...], onehot)
        weight_ref[...] = dot(radial, hidden_ref[:, span])
        _, _, x_row, y_row, z_row = unit(vec_ref[:, span])
        q_rows = harmonics(x_row, y_row, z_row)
        height, width = 16, 128
        for lane in range(0, block, width):
            cols = slice(lane, lane + width)

            def wide(row):
                return jnp.broadcast_to(row[:, cols], (height, width))

            x, y, z = wide(x_row), wide(y_row), wide(z_row)
            q = [wide(row) for row in q_rows]
            hx, hy, hz = half_root * x, half_root * y, half_root * z
            for low in range(0, chans, height):

                def at(ref, k):
                    return ref[k * chans + low : k * chans + low + height, cols]

                def put(k, value):
                    mess_ref[k * chans + low : k * chans + low + height, cols] = value.astype(bf16)

                s = at(source_ref, 0)
                v = [at(source_ref, k) for k in (1, 2, 3)]
                t = [at(source_ref, k) for k in (4, 5, 6, 7, 8)]
                along = v[0] * x + v[1] * y + v[2] * z
                tq = t[0] * q[0] + t[1] * q[1] + t[2] * q[2] + t[3] * q[3] + t[4] * q[4]
                put(0, at(weight_ref, 0) * s + at(weight_ref, 1) * tq + at(weight_ref, 2) * along)
                ws = at(weight_ref, 3) * s
                w4, w5, w6 = at(weight_ref, 4), at(weight_ref, 5), at(weight_ref, 6)
                cross = [
                    v[1] * z - v[2] * y,
                    v[2] * x - v[0] * z,
                    v[0] * y - v[1] * x,
                ]
                t3 = 0.5 * t[2]
                grad = [
                    hy * t[0] - x * t3 + hz * t[3] + hx * t[4],
                    hx * t[0] + hz * t[1] - y * t3 - hy * t[4],
                    hy * t[1] + z * t[2] + hx * t[3],
                ]
                for k, part in enumerate((x, y, z)):
                    put(1 + k, ws * part + w4 * v[k] + w5 * cross[k] + w6 * grad[k])
                ws = at(weight_ref, 7) * s
                w8, w9 = at(weight_ref, 8), at(weight_ref, 9)
                sym = [
                    hy * v[0] + hx * v[1],
                    hz * v[1] + hy * v[2],
                    1.5 * v[2] * z - 0.5 * along,
                    hz * v[0] + hx * v[2],
                    hx * v[0] - hy * v[1],
                ]
                for k in range(5):
                    put(4 + k, ws * q[k] + w8 * t[k] + w9 * sym[k])
        lanes = lax.broadcasted_iota(jnp.int32, (1, block), 1) + offset
        target = jnp.where(lanes < live, edges_ref[1:2, span], -1)
        acc_ref[...] += dot_nt(mess_ref[...], onehot_rows(target, atoms))

    def run(table, edges_ref, vec_ref, hidden_ref, live):
        def body(step, carry):
            visit(table, edges_ref, vec_ref, hidden_ref, live, step)
            return carry

        lax.fori_loop(0, lax.div(live + (block - 1), block), body, 0)

    run(table_ref, inner_edges_ref, inner_vec_ref, inner_hidden_ref, count_ref[0, 0])
    run(halo_table_ref, outer_edges_ref, outer_vec_ref, outer_hidden_ref, count_ref[0, 1])
    out_ref[...] = (acc_ref[...] * neighbour_norm).astype(bf16)


mesh_ids = pl.DeviceIdType.MESH


def greet(peers):
    barrier = pltpu.get_barrier_semaphore()
    for peer in peers:
        pl.semaphore_signal(barrier, inc=1, device_id=peer, device_id_type=mesh_ids)
    pl.semaphore_wait(barrier, len(peers))


def others(axis, total):
    me = lax.axis_index(axis)
    return [{axis: lax.rem(me + step, total)} for step in range(1, total)]


def beside(total):
    me = lax.axis_index("slab")
    return {"slab": lax.rem(me + total - 1, total)}, {"slab": lax.rem(me + 1, total)}


def send_halo(send_ref, land_ref, send_sem, recv_sem, total):
    copies = []
    for side, peer in enumerate(beside(total)):
        copies.append(
            pltpu.make_async_remote_copy(
                src_ref=send_ref.at[side],
                dst_ref=land_ref.at[1 - side],
                send_sem=send_sem.at[side],
                recv_sem=recv_sem.at[side],
                device_id=peer,
                device_id_type=mesh_ids,
            )
        )
    for copy in copies:
        copy.start()
    return copies


def species_kernel(slabs, species_ref, halo_ref, out_ref, send_ref, land_ref, send_sem, recv_sem):
    values = jnp.broadcast_to(species_ref[...].astype(f32), (16, species_ref.shape[1])).astype(bf16)
    for side in range(2):
        onehot = onehot_rows(halo_ref[side : side + 1], species_ref.shape[1])
        send_ref[side] = dot(values, onehot)[0:8]
    greet(beside(slabs))
    for copy in send_halo(send_ref, land_ref, send_sem, recv_sem, slabs):
        copy.wait()
    out_ref[...] = jnp.concatenate([land_ref[0, 0:1], land_ref[1, 0:1]], axis=1).astype(jnp.int32)


def exchange(agg_ref, all_ref, send_sem, recv_sem, total):
    part = agg_ref.shape[0] // 9
    me = lax.axis_index("chan")
    peers = others("chan", total)
    copies = []
    for k in range(9):
        span = slice(k * part, (k + 1) * part)
        for i, peer in enumerate(peers):
            copies.append(
                pltpu.make_async_remote_copy(
                    src_ref=agg_ref.at[span],
                    dst_ref=all_ref.at[me, span],
                    send_sem=send_sem.at[i, k],
                    recv_sem=recv_sem.at[i, k],
                    device_id=peer,
                    device_id_type=mesh_ids,
                )
            )
    for copy in copies:
        copy.start()
    all_ref[me] = agg_ref[...]

    def component(k):
        for copy in copies[k * len(peers) : (k + 1) * len(peers)]:
            copy.wait_recv()
        span = slice(k * part, (k + 1) * part)
        return jnp.concatenate([all_ref[i, span] for i in range(total)], axis=0)

    return copies, component


class Updates:
    def __init__(self, component, layer, scalar_ref, irrep_ref):
        self.component, self.layer, self.irrep = component, layer, irrep_ref
        chans = irrep_ref.shape[2]
        y = dot(turned(scalar_ref[layer]), component(0))
        self.scalar = silu(y[:chans])
        self.gates = sigmoid(y[chans : 2 * chans]), sigmoid(y[2 * chans :])

    def __getitem__(self, k):
        if k == 0:
            return self.scalar
        kind = 0 if k < 4 else 1
        return self.gates[kind] * dot(self.irrep[self.layer, kind], self.component(k))


def middle_kernel(
    slabs,
    parts,
    species_ref,
    halo_ref,
    agg_ref,
    embed_ref,
    mix_ref,
    scalar_ref,
    irrep_ref,
    state_ref,
    table_ref,
    halo_table_ref,
    all_ref,
    send_ref,
    land_ref,
    agg_send,
    agg_recv,
    halo_send,
    halo_recv,
):
    part = mix_ref.shape[2]
    greet(others("chan", parts) + list(beside(slabs)))
    copies, component = exchange(agg_ref, all_ref, agg_send, agg_recv, parts)
    onehots = jnp.concatenate(
        [onehot_rows(halo_ref[side : side + 1], table_ref.shape[1]) for side in range(2)], axis=1
    )
    start = initial(embed_ref, species_ref[...])
    outs = Updates(component, 0, scalar_ref, irrep_ref)
    held = halo_ref.shape[1]
    for k in range(9):
        out = outs[k]
        if k == 0:
            out += start
        state_ref[k] = out
        which = 0 if k == 0 else (1 if k < 4 else 2)
        span = slice(k * part, (k + 1) * part)
        mixed = dot(mix_ref[1, which], out.astype(bf16)).astype(bf16)
        table_ref[span] = mixed
        picked = dot(mixed, onehots).astype(bf16)
        for side in range(2):
            send_ref[side, span] = picked[:, side * held : (side + 1) * held]
    for copy in copies:
        copy.wait_send()
    for copy in send_halo(send_ref, land_ref, halo_send, halo_recv, slabs):
        copy.wait()
    for side in range(2):
        halo_table_ref[:, side * held : (side + 1) * held] = land_ref[side]


def last_kernel(
    slabs,
    parts,
    species_ref,
    count_ref,
    agg_ref,
    state_in_ref,
    scalar_ref,
    irrep_ref,
    readout_ref,
    energy_ref,
    state_ref,
    atom_ref,
    mean_ref,
    all_ref,
    energies_ref,
    agg_send,
    agg_recv,
    energy_send,
    energy_recv,
):
    peers = others("slab", slabs)
    greet(others("chan", parts) + peers)
    copies, component = exchange(agg_ref, all_ref, agg_send, agg_recv, parts)
    chans, atoms = state_ref.shape[1:]
    lines = lax.broadcasted_iota(jnp.int32, (chans, chans), 0)
    across = lax.broadcasted_iota(jnp.int32, (chans, chans), 1)
    readout = jnp.sum(
        jnp.where(lines == across, readout_ref[...], 0.0), axis=1, keepdims=True
    )
    own = jnp.zeros((1, atoms), f32)
    for kind in range(energy_ref.shape[0]):
        own = jnp.where(species_ref[...] == kind, energy_ref[kind], own)
    lanes = lax.broadcasted_iota(jnp.int32, (1, atoms), 1)
    live = lanes < count_ref[0]
    outs = Updates(component, 1, scalar_ref, irrep_ref)
    out = state_in_ref[0] + outs[0]
    state_ref[0] = out
    total = jnp.where(live, jnp.sum(out * readout, axis=0, keepdims=True) + own, 0.0)
    atom_ref[...] = total
    me = lax.axis_index("slab")
    energies_ref[me] = jnp.broadcast_to(
        jnp.sum(total, axis=1, keepdims=True), energies_ref.shape[1:]
    )
    for k in range(1, 4):
        state_ref[k] = state_in_ref[k] + outs[k]
    sums = [
        pltpu.make_async_remote_copy(
            src_ref=energies_ref.at[me],
            dst_ref=energies_ref.at[me],
            send_sem=energy_send.at[i],
            recv_sem=energy_recv.at[i],
            device_id=peer,
            device_id_type=mesh_ids,
        )
        for i, peer in enumerate(peers)
    ]
    for copy in sums:
        copy.start()
    for k in range(4, 9):
        state_ref[k] = state_in_ref[k] + outs[k]
    for copy in copies:
        copy.wait_send()
    for copy in sums:
        copy.wait()
    mean_ref[...] = jnp.sum(energies_ref[...], axis=0)[0:1, 0:1] * (1.0 / (atoms * slabs))


vmem = pl.BlockSpec(memory_space=pltpu.VMEM)
smem = pl.BlockSpec(memory_space=pltpu.SMEM)
params = pltpu.CompilerParams(vmem_limit_bytes=56 * 1024 * 1024)


def remote(number):
    return pltpu.CompilerParams(
        vmem_limit_bytes=56 * 1024 * 1024, collective_id=number, has_side_effects=True
    )


def local(
    species,
    atom_count,
    halo_index,
    edge_count,
    inner_edges,
    outer_edges,
    inner_vec,
    outer_vec,
    embed_table,
    radial_in,
    radial_mid,
    radial_out,
    mix_in,
    mix_scalar,
    mix_irrep,
    readout,
    species_energy,
):
    slabs = lax.axis_size("slab")
    parts = lax.axis_size("chan")
    atoms = species.shape[0]
    chans = embed_table.shape[0]
    part = mix_in.shape[2]
    breadth = radial_mid.shape[1]
    basis = radial_in.shape[2]
    paths = radial_out.shape[1]
    halo = halo_index[0]
    held = halo.shape[1]
    rows = 9 * part
    dma = pltpu.SemaphoreType.DMA
    species_row = species[None, :]
    embed = embed_table.T
    scalar = jnp.swapaxes(mix_scalar, 1, 2)
    halo_species = pl.pallas_call(
        functools.partial(species_kernel, slabs),
        out_shape=jax.ShapeDtypeStruct((1, 2 * held), jnp.int32),
        in_specs=[vmem] * 2,
        out_specs=vmem,
        scratch_shapes=[
            pltpu.VMEM((2, 8, held), f32),
            pltpu.VMEM((2, 8, held), f32),
            dma((2,)),
            dma((2,)),
        ],
        compiler_params=remote(0),
        name="halo_species",
    )(species_row, halo)
    block = math.gcd(BLOCK, math.gcd(inner_edges.shape[1], outer_edges.shape[1]))
    agg, inner_hidden, outer_hidden = pl.pallas_call(
        functools.partial(first_kernel, block),
        out_shape=(
            jax.ShapeDtypeStruct((rows, atoms), bf16),
            jax.ShapeDtypeStruct((breadth, inner_edges.shape[1]), bf16),
            jax.ShapeDtypeStruct((breadth, outer_edges.shape[1]), bf16),
        ),
        in_specs=[smem] + [vmem] * 11,
        out_specs=(vmem, vmem, vmem),
        scratch_shapes=[
            pltpu.VMEM((rows, atoms), f32),
            pltpu.VMEM((2, part, atoms), bf16),
            pltpu.VMEM((rows, block), bf16),
            pltpu.VMEM((2 * breadth, basis), bf16),
            pltpu.VMEM((2 * breadth, 2 * breadth), bf16),
            pltpu.VMEM((3 * part, breadth), bf16),
        ],
        compiler_params=params,
        name="first_layer",
    )(
        edge_count,
        species_row,
        halo_species,
        inner_edges,
        outer_edges,
        inner_vec,
        outer_vec,
        embed,
        mix_in,
        jnp.swapaxes(radial_in, 1, 2),
        radial_mid,
        radial_out,
    )
    state, table, halo_table = pl.pallas_call(
        functools.partial(middle_kernel, slabs, parts),
        out_shape=(
            jax.ShapeDtypeStruct((9, chans, atoms), f32),
            jax.ShapeDtypeStruct((rows, atoms), bf16),
            jax.ShapeDtypeStruct((rows, 2 * held), bf16),
        ),
        in_specs=[vmem] * 7,
        out_specs=(vmem, vmem, vmem),
        scratch_shapes=[
            pltpu.VMEM((parts, rows, atoms), bf16),
            pltpu.VMEM((2, rows, held), bf16),
            pltpu.VMEM((2, rows, held), bf16),
            dma((parts - 1, 9)),
            dma((parts - 1, 9)),
            dma((2,)),
            dma((2,)),
        ],
        compiler_params=remote(1),
        name="middle",
    )(species_row, halo, agg, embed, mix_in, scalar, mix_irrep)
    agg = pl.pallas_call(
        functools.partial(second_kernel, block),
        out_shape=jax.ShapeDtypeStruct((rows, atoms), bf16),
        in_specs=[smem] + [vmem] * 9,
        out_specs=vmem,
        scratch_shapes=[
            pltpu.VMEM((rows, atoms), f32),
            pltpu.VMEM((paths * part, block), f32),
            pltpu.VMEM((rows, block), f32),
            pltpu.VMEM((rows, block), bf16),
        ],
        compiler_params=params,
        name="second_layer",
    )(
        edge_count,
        table,
        halo_table,
        inner_edges,
        outer_edges,
        inner_vec,
        outer_vec,
        inner_hidden,
        outer_hidden,
        radial_out,
    )
    node_state, atom_energy, mean_energy = pl.pallas_call(
        functools.partial(last_kernel, slabs, parts),
        out_shape=(
            jax.ShapeDtypeStruct((9, chans, atoms), f32),
            jax.ShapeDtypeStruct((1, atoms), f32),
            jax.ShapeDtypeStruct((1, 1), f32),
        ),
        in_specs=[vmem, smem] + [vmem] * 5 + [smem],
        out_specs=(vmem, vmem, vmem),
        scratch_shapes=[
            pltpu.VMEM((parts, rows, atoms), bf16),
            pltpu.VMEM((slabs, 8, 128), f32),
            dma((parts - 1, 9)),
            dma((parts - 1, 9)),
            dma((slabs - 1,)),
            dma((slabs - 1,)),
        ],
        compiler_params=remote(2),
        name="last",
    )(
        species_row,
        atom_count,
        agg,
        state,
        scalar,
        mix_irrep,
        readout[None, :],
        species_energy,
    )
    return (node_state, atom_energy[0], mean_energy[0, 0])


def solution(mesh):
    return jax.shard_map(
        local,
        mesh=mesh,
        in_specs=(
            P("slab"),
            P("slab"),
            P("slab", None, None),
            P("slab", None),
            P(None, "slab"),
            P(None, "slab"),
            P(None, "slab"),
            P(None, "slab"),
            P(),
            P(),
            P(),
            P(None, None, "chan", None),
            P(None, None, "chan", None),
            P(),
            P(),
            P(),
            P(),
        ),
        out_specs=(P(None, None, "slab"), P("slab"), P()),
        check_vma=False,
    )
```

```python
import functools
import math

import jax
import jax.numpy as jnp
from jax import lax
from jax.experimental import pallas as pl
from jax.experimental.pallas import tpu as pltpu
from jax.sharding import PartitionSpec as P

cutoff = 5.0
neighbour_norm = 1.0 / math.sqrt(48.0)
root_three = math.sqrt(3.0)
half_root = 0.5 * math.sqrt(3.0)
BLOCK = 1024
f32 = jnp.float32
bf16 = jnp.bfloat16


def dot(a, b):
    return jnp.dot(a, b, preferred_element_type=f32)


def dot_nt(a, b):
    return lax.dot_general(a, b, (((1,), (1,)), ((), ())), preferred_element_type=f32)


def sigmoid(v):
    return 0.5 * jnp.tanh(0.5 * v) + 0.5


def silu(v):
    half = 0.5 * v
    return half * jnp.tanh(half) + half


def onehot_rows(index, rows):
    slots = lax.broadcasted_iota(jnp.int32, (rows, index.shape[1]), 0)
    return jnp.where(slots == index, 1.0, 0.0).astype(bf16)


def turned(matrix):
    return matrix.astype(f32).T.astype(bf16)


def initial(embed_ref, species_row):
    return dot(turned(embed_ref[...]), onehot_rows(species_row, embed_ref.shape[0]))


def unit(vec):
    x, y, z = vec[0:1], vec[1:2], vec[2:3]
    squared = x * x + y * y + z * z
    inverse = lax.rsqrt(squared + 0.25)
    return squared, inverse, x * inverse, y * inverse, z * inverse


def bessel_rows(squared, inverse, orders):
    length = jnp.sqrt(squared)
    fraction = jnp.minimum(length * (1.0 / cutoff), 1.0)
    cube = fraction * fraction * fraction
    sixth = cube * cube
    envelope = 1.0 - sixth * (28.0 - fraction * (48.0 - 21.0 * fraction))
    half = length * (0.5 * math.pi / cutoff)
    h2 = half * half
    sine = 1.0
    cosine = 1.0
    for order in range(12, 0, -2):
        sine = 1.0 - sine * h2 * (1.0 / ((order + 1) * order))
        cosine = 1.0 - cosine * h2 * (1.0 / (order * (order - 1)))
    sine = sine * half
    twice_cos = 2.0 - 4.0 * sine * sine
    first = 2.0 * sine * cosine
    scale = math.sqrt(2.0 / cutoff) * inverse * envelope
    before, now = jnp.zeros_like(first), first * scale
    rows = []
    for _ in range(orders):
        rows.append(now)
        before, now = now, twice_cos * now - before
    return jnp.concatenate(rows, axis=0)


def harmonics(x, y, z):
    return [
        root_three * x * y,
        root_three * y * z,
        0.5 * (2.0 * z * z - x * x - y * y),
        root_three * x * z,
        half_root * (x * x - y * y),
    ]


def radial(entry, mid, basis):
    hidden = silu(dot(entry, basis)).astype(bf16)
    return silu(dot(mid, hidden)).astype(bf16)


def first_kernel(
    block,
    count_ref,
    species_ref,
    halo_species_ref,
    inner_edges_ref,
    outer_edges_ref,
    inner_vec_ref,
    outer_vec_ref,
    embed_ref,
    mix_ref,
    radial_in_ref,
    radial_mid_ref,
    radial_out_ref,
    agg_ref,
    inner_basis_ref,
    outer_basis_ref,
    acc_ref,
    table_ref,
    mess_ref,
    entry_ref,
    paths_ref,
):
    chans = mix_ref.shape[2]
    atoms = species_ref.shape[1]
    for slot, ref in enumerate((species_ref, halo_species_ref)):
        init = initial(embed_ref, ref[...]).astype(bf16)
        table_ref[slot] = dot(mix_ref[0, 0], init).astype(bf16)
    acc_ref[...] = jnp.zeros_like(acc_ref)
    entry_ref[...] = turned(radial_in_ref[0])
    for k, path in enumerate((0, 3, 7)):
        paths_ref[k * chans : (k + 1) * chans] = radial_out_ref[0, path]

    def visit(slot, edges_ref, vec_ref, basis_ref, live, step):
        offset = pl.multiple_of(step * block, block)
        span = pl.ds(offset, block)
        source = onehot_rows(edges_ref[0:1, span], table_ref.shape[2])
        gathered = dot(table_ref[slot], source)
        squared, inverse, x, y, z = unit(vec_ref[:, span])
        basis = bessel_rows(squared, inverse, radial_in_ref.shape[1]).astype(bf16)
        basis_ref[:, span] = basis
        weights = dot(paths_ref[...], radial(entry_ref[...], radial_mid_ref[0], basis))
        q = harmonics(x, y, z)
        lanes = lax.broadcasted_iota(jnp.int32, (1, block), 1) + offset
        target = jnp.where(lanes < live, edges_ref[1:2, span], -1)
        by_vector = weights[chans : 2 * chans] * gathered
        by_tensor = weights[2 * chans : 3 * chans] * gathered
        mess_ref[0:chans] = (weights[0:chans] * gathered).astype(bf16)
        for k, part in enumerate((x, y, z)):
            mess_ref[(1 + k) * chans : (2 + k) * chans] = (by_vector * part).astype(bf16)
        for k, part in enumerate(q):
            mess_ref[(4 + k) * chans : (5 + k) * chans] = (by_tensor * part).astype(bf16)
        acc_ref[...] += dot_nt(mess_ref[...], onehot_rows(target, atoms))

    def run(slot, edges_ref, vec_ref, basis_ref, live):
        def body(step, carry):
            visit(slot, edges_ref, vec_ref, basis_ref, live, step)
            return carry

        lax.fori_loop(0, lax.div(live + (block - 1), block), body, 0)

    run(0, inner_edges_ref, inner_vec_ref, inner_basis_ref, count_ref[0, 0])
    run(1, outer_edges_ref, outer_vec_ref, outer_basis_ref, count_ref[0, 1])
    agg_ref[...] = (acc_ref[...] * neighbour_norm).astype(bf16)


def second_kernel(
    block,
    count_ref,
    table_ref,
    halo_table_ref,
    inner_edges_ref,
    outer_edges_ref,
    inner_vec_ref,
    outer_vec_ref,
    inner_hidden_ref,
    outer_hidden_ref,
    radial_out_ref,
    out_ref,
    acc_ref,
    weight_ref,
    source_ref,
    mess_ref,
    inner_held_ref,
    outer_held_ref,
    inner_sem,
    outer_sem,
):
    chans = table_ref.shape[0] // 9
    atoms = out_ref.shape[1]
    lists = (
        (inner_hidden_ref, inner_held_ref, inner_sem, count_ref[0, 0]),
        (outer_hidden_ref, outer_held_ref, outer_sem, count_ref[0, 1]),
    )

    def fetch(hidden_ref, held_ref, sem, step):
        span = pl.ds(pl.multiple_of(step * block, block), block)
        return pltpu.make_async_copy(hidden_ref.at[:, span], held_ref.at[:, span], sem.at[step])

    for hidden_ref, held_ref, sem, live in lists:

        def begin(step, carry, hidden_ref=hidden_ref, held_ref=held_ref, sem=sem):
            fetch(hidden_ref, held_ref, sem, step).start()
            return carry

        lax.fori_loop(0, lax.div(live + (block - 1), block), begin, 0)
    acc_ref[...] = jnp.zeros_like(acc_ref)
    paths, _, breadth = radial_out_ref.shape[1:]
    radial = radial_out_ref[1].reshape(paths * chans, breadth)

    def visit(table_ref, edges_ref, vec_ref, held, step):
        hidden_ref, held_ref, sem, live = held
        fetch(hidden_ref, held_ref, sem, step).wait()
        offset = pl.multiple_of(step * block, block)
        span = pl.ds(offset, block)
        onehot = onehot_rows(edges_ref[0:1, span], table_ref.shape[1])
        source_ref[...] = dot(table_ref[...], onehot)
        weight_ref[...] = dot(radial, held_ref[:, span])
        _, _, x_row, y_row, z_row = unit(vec_ref[:, span])
        q_rows = harmonics(x_row, y_row, z_row)
        height, width = 16, 128
        for lane in range(0, block, width):
            cols = slice(lane, lane + width)

            def wide(row):
                return jnp.broadcast_to(row[:, cols], (height, width))

            x, y, z = wide(x_row), wide(y_row), wide(z_row)
            q = [wide(row) for row in q_rows]
            hx, hy, hz = half_root * x, half_root * y, half_root * z
            for low in range(0, chans, height):

                def at(ref, k):
                    return ref[k * chans + low : k * chans + low + height, cols]

                def put(k, value):
                    mess_ref[k * chans + low : k * chans + low + height, cols] = value.astype(bf16)

                s = at(source_ref, 0)
                v = [at(source_ref, k) for k in (1, 2, 3)]
                t = [at(source_ref, k) for k in (4, 5, 6, 7, 8)]
                along = v[0] * x + v[1] * y + v[2] * z
                tq = t[0] * q[0] + t[1] * q[1] + t[2] * q[2] + t[3] * q[3] + t[4] * q[4]
                put(0, at(weight_ref, 0) * s + at(weight_ref, 1) * tq + at(weight_ref, 2) * along)
                ws = at(weight_ref, 3) * s
                w4, w5, w6 = at(weight_ref, 4), at(weight_ref, 5), at(weight_ref, 6)
                cross = [
                    v[1] * z - v[2] * y,
                    v[2] * x - v[0] * z,
                    v[0] * y - v[1] * x,
                ]
                t3 = 0.5 * t[2]
                grad = [
                    hy * t[0] - x * t3 + hz * t[3] + hx * t[4],
                    hx * t[0] + hz * t[1] - y * t3 - hy * t[4],
                    hy * t[1] + z * t[2] + hx * t[3],
                ]
                for k, part in enumerate((x, y, z)):
                    put(1 + k, ws * part + w4 * v[k] + w5 * cross[k] + w6 * grad[k])
                ws = at(weight_ref, 7) * s
                w8, w9 = at(weight_ref, 8), at(weight_ref, 9)
                sym = [
                    hy * v[0] + hx * v[1],
                    hz * v[1] + hy * v[2],
                    1.5 * v[2] * z - 0.5 * along,
                    hz * v[0] + hx * v[2],
                    hx * v[0] - hy * v[1],
                ]
                for k in range(5):
                    put(4 + k, ws * q[k] + w8 * t[k] + w9 * sym[k])
        lanes = lax.broadcasted_iota(jnp.int32, (1, block), 1) + offset
        target = jnp.where(lanes < live, edges_ref[1:2, span], -1)
        acc_ref[...] += dot_nt(mess_ref[...], onehot_rows(target, atoms))

    def run(table, edges_ref, vec_ref, held):
        def body(step, carry):
            visit(table, edges_ref, vec_ref, held, step)
            return carry

        lax.fori_loop(0, lax.div(held[3] + (block - 1), block), body, 0)

    run(table_ref, inner_edges_ref, inner_vec_ref, lists[0])
    run(halo_table_ref, outer_edges_ref, outer_vec_ref, lists[1])
    out_ref[...] = (acc_ref[...] * neighbour_norm).astype(bf16)


mesh_ids = pl.DeviceIdType.MESH


def greet(peers):
    barrier = pltpu.get_barrier_semaphore()
    for peer in peers:
        pl.semaphore_signal(barrier, inc=1, device_id=peer, device_id_type=mesh_ids)
    pl.semaphore_wait(barrier, len(peers))


def others(axis, total):
    me = lax.axis_index(axis)
    return [{axis: lax.rem(me + step, total)} for step in range(1, total)]


def beside(total):
    me = lax.axis_index("slab")
    return {"slab": lax.rem(me + total - 1, total)}, {"slab": lax.rem(me + 1, total)}


def send_halo(send_ref, land_ref, send_sem, recv_sem, total):
    copies = []
    for side, peer in enumerate(beside(total)):
        copies.append(
            pltpu.make_async_remote_copy(
                src_ref=send_ref.at[side],
                dst_ref=land_ref.at[1 - side],
                send_sem=send_sem.at[side],
                recv_sem=recv_sem.at[side],
                device_id=peer,
                device_id_type=mesh_ids,
            )
        )
    for copy in copies:
        copy.start()
    return copies


def species_kernel(slabs, species_ref, halo_ref, out_ref, send_ref, land_ref, send_sem, recv_sem):
    values = jnp.broadcast_to(species_ref[...].astype(f32), (16, species_ref.shape[1])).astype(bf16)
    for side in range(2):
        onehot = onehot_rows(halo_ref[side : side + 1], species_ref.shape[1])
        send_ref[side] = dot(values, onehot)[0:8]
    greet(beside(slabs))
    for copy in send_halo(send_ref, land_ref, send_sem, recv_sem, slabs):
        copy.wait()
    out_ref[...] = jnp.concatenate([land_ref[0, 0:1], land_ref[1, 0:1]], axis=1).astype(jnp.int32)


def exchange(agg_ref, all_ref, send_sem, recv_sem, total):
    part = agg_ref.shape[0] // 9
    me = lax.axis_index("chan")
    peers = others("chan", total)
    copies = []
    for k in range(9):
        span = slice(k * part, (k + 1) * part)
        for i, peer in enumerate(peers):
            copies.append(
                pltpu.make_async_remote_copy(
                    src_ref=agg_ref.at[span],
                    dst_ref=all_ref.at[me, span],
                    send_sem=send_sem.at[i, k],
                    recv_sem=recv_sem.at[i, k],
                    device_id=peer,
                    device_id_type=mesh_ids,
                )
            )
    for copy in copies:
        copy.start()
    all_ref[me] = agg_ref[...]

    def component(k):
        for copy in copies[k * len(peers) : (k + 1) * len(peers)]:
            copy.wait_recv()
        span = slice(k * part, (k + 1) * part)
        return jnp.concatenate([all_ref[i, span] for i in range(total)], axis=0)

    return copies, component


class Updates:
    def __init__(self, component, layer, scalar_ref, irrep_ref):
        self.component, self.layer, self.irrep = component, layer, irrep_ref
        chans = irrep_ref.shape[2]
        y = dot(turned(scalar_ref[layer]), component(0))
        self.scalar = silu(y[:chans])
        self.gates = sigmoid(y[chans : 2 * chans]), sigmoid(y[2 * chans :])

    def __getitem__(self, k):
        if k == 0:
            return self.scalar
        kind = 0 if k < 4 else 1
        return self.gates[kind] * dot(self.irrep[self.layer, kind], self.component(k))


def middle_kernel(
    slabs,
    parts,
    block,
    species_ref,
    halo_ref,
    agg_ref,
    embed_ref,
    mix_ref,
    scalar_ref,
    irrep_ref,
    inner_basis_ref,
    outer_basis_ref,
    radial_in_ref,
    radial_mid_ref,
    state_ref,
    scalars_ref,
    table_ref,
    halo_table_ref,
    inner_hidden_ref,
    outer_hidden_ref,
    inner_held_ref,
    outer_held_ref,
    out_sem,
    all_ref,
    send_ref,
    land_ref,
    agg_send,
    agg_recv,
    halo_send,
    halo_recv,
):
    part = mix_ref.shape[2]
    greet(others("chan", parts) + list(beside(slabs)))
    copies, component = exchange(agg_ref, all_ref, agg_send, agg_recv, parts)
    entry = turned(radial_in_ref[1])
    writes = []
    lists = (
        (inner_basis_ref, inner_held_ref, inner_hidden_ref),
        (outer_basis_ref, outer_held_ref, outer_hidden_ref),
    )
    for i, (basis_ref, held_ref, hidden_ref) in enumerate(lists):

        def body(step, carry, basis_ref=basis_ref, held_ref=held_ref):
            span = pl.ds(pl.multiple_of(step * block, block), block)
            held_ref[:, span] = radial(entry, radial_mid_ref[1], basis_ref[:, span])
            return carry

        lax.fori_loop(0, basis_ref.shape[1] // block, body, 0)
        writes.append(pltpu.make_async_copy(held_ref, hidden_ref, out_sem.at[i]))
    onehots = jnp.concatenate(
        [onehot_rows(halo_ref[side : side + 1], table_ref.shape[1]) for side in range(2)], axis=1
    )
    start = initial(embed_ref, species_ref[...])
    outs = Updates(component, 0, scalar_ref, irrep_ref)
    held = halo_ref.shape[1]
    for k in range(9):
        out = outs[k]
        if k == 0:
            for write in writes:
                write.start()
            out += start
            scalars_ref[...] = out
        state_ref[k] = out
        which = 0 if k == 0 else (1 if k < 4 else 2)
        span = slice(k * part, (k + 1) * part)
        mixed = dot(mix_ref[1, which], out.astype(bf16)).astype(bf16)
        table_ref[span] = mixed
        picked = dot(mixed, onehots).astype(bf16)
        for side in range(2):
            send_ref[side, span] = picked[:, side * held : (side + 1) * held]
    for copy in copies:
        copy.wait_send()
    for copy in send_halo(send_ref, land_ref, halo_send, halo_recv, slabs):
        copy.wait()
    for write in writes:
        write.wait()
    for side in range(2):
        halo_table_ref[:, side * held : (side + 1) * held] = land_ref[side]


def energy_kernel(
    slabs,
    parts,
    species_ref,
    count_ref,
    agg_ref,
    scalars_ref,
    scalar_ref,
    readout_ref,
    energy_ref,
    every_ref,
    atom_ref,
    mean_ref,
    all_ref,
    energies_ref,
    agg_send,
    agg_recv,
    energy_send,
    energy_recv,
):
    peers = others("slab", slabs)
    greet(others("chan", parts) + peers)
    copies, component = exchange(agg_ref, all_ref, agg_send, agg_recv, parts)
    chans, atoms = scalars_ref.shape
    lines = lax.broadcasted_iota(jnp.int32, (chans, chans), 0)
    across = lax.broadcasted_iota(jnp.int32, (chans, chans), 1)
    readout = jnp.sum(jnp.where(lines == across, readout_ref[...], 0.0), axis=1, keepdims=True)
    own = jnp.zeros((1, atoms), f32)
    for kind in range(energy_ref.shape[0]):
        own = jnp.where(species_ref[...] == kind, energy_ref[kind], own)
    lanes = lax.broadcasted_iota(jnp.int32, (1, atoms), 1)
    weight = turned(scalar_ref[1])[:chans]
    out = scalars_ref[...] + silu(dot(weight, component(0)))
    total = jnp.sum(out * readout, axis=0, keepdims=True) + own
    total = jnp.where(lanes < count_ref[0], total, 0.0)
    me = lax.axis_index("slab")
    energies_ref[me] = jnp.broadcast_to(
        jnp.sum(total, axis=1, keepdims=True), energies_ref.shape[1:]
    )
    atom_ref[...] = total
    part = agg_ref.shape[0] // 9
    every_ref[:, :part] = all_ref[:, :part]
    sums = [
        pltpu.make_async_remote_copy(
            src_ref=energies_ref.at[me],
            dst_ref=energies_ref.at[me],
            send_sem=energy_send.at[i],
            recv_sem=energy_recv.at[i],
            device_id=peer,
            device_id_type=mesh_ids,
        )
        for i, peer in enumerate(peers)
    ]
    for copy in sums:
        copy.start()
    for k in range(1, 9):
        component(k)
    every_ref[:, part:] = all_ref[:, part:]
    for copy in copies:
        copy.wait_send()
    for copy in sums:
        copy.wait()
    mean_ref[...] = jnp.sum(energies_ref[...], axis=0)[0:1, 0:1] * (1.0 / (atoms * slabs))


def last_kernel(
    every_ref, state_in_ref, scalar_ref, irrep_ref, atom_in_ref, mean_in_ref, state_ref, atom_ref, mean_ref
):
    part = every_ref.shape[1] // 9

    def component(k):
        span = slice(k * part, (k + 1) * part)
        return jnp.concatenate([every_ref[i, span] for i in range(every_ref.shape[0])], axis=0)

    outs = Updates(component, 1, scalar_ref, irrep_ref)
    for k in range(9):
        state_ref[k] = state_in_ref[k] + outs[k]
    atom_ref[...] = atom_in_ref[...]
    mean_ref[...] = mean_in_ref[...]


vmem = pl.BlockSpec(memory_space=pltpu.VMEM)
anywhere = pl.BlockSpec(memory_space=pl.ANY)
smem = pl.BlockSpec(memory_space=pltpu.SMEM)
params = pltpu.CompilerParams(vmem_limit_bytes=56 * 1024 * 1024)


def remote(number):
    return pltpu.CompilerParams(
        vmem_limit_bytes=56 * 1024 * 1024, collective_id=number, has_side_effects=True
    )


def local(
    species,
    atom_count,
    halo_index,
    edge_count,
    inner_edges,
    outer_edges,
    inner_vec,
    outer_vec,
    embed_table,
    radial_in,
    radial_mid,
    radial_out,
    mix_in,
    mix_scalar,
    mix_irrep,
    readout,
    species_energy,
):
    slabs = lax.axis_size("slab")
    parts = lax.axis_size("chan")
    atoms = species.shape[0]
    chans = embed_table.shape[0]
    part = mix_in.shape[2]
    breadth = radial_mid.shape[1]
    basis = radial_in.shape[2]
    paths = radial_out.shape[1]
    halo = halo_index[0]
    held = halo.shape[1]
    rows = 9 * part
    dma = pltpu.SemaphoreType.DMA
    species_row = species[None, :]
    embed = embed_table.T
    scalar = jnp.swapaxes(mix_scalar, 1, 2)
    halo_species = pl.pallas_call(
        functools.partial(species_kernel, slabs),
        out_shape=jax.ShapeDtypeStruct((1, 2 * held), jnp.int32),
        in_specs=[vmem] * 2,
        out_specs=vmem,
        scratch_shapes=[
            pltpu.VMEM((2, 8, held), f32),
            pltpu.VMEM((2, 8, held), f32),
            dma((2,)),
            dma((2,)),
        ],
        compiler_params=remote(0),
        name="halo_species",
    )(species_row, halo)
    block = math.gcd(BLOCK, math.gcd(inner_edges.shape[1], outer_edges.shape[1]))
    inner_total, outer_total = inner_edges.shape[1], outer_edges.shape[1]
    radial_turned = jnp.swapaxes(radial_in, 1, 2)
    agg, inner_basis, outer_basis = pl.pallas_call(
        functools.partial(first_kernel, block),
        out_shape=(
            jax.ShapeDtypeStruct((rows, atoms), bf16),
            jax.ShapeDtypeStruct((basis, inner_total), bf16),
            jax.ShapeDtypeStruct((basis, outer_total), bf16),
        ),
        in_specs=[smem] + [vmem] * 11,
        out_specs=(vmem, vmem, vmem),
        scratch_shapes=[
            pltpu.VMEM((rows, atoms), f32),
            pltpu.VMEM((2, part, atoms), bf16),
            pltpu.VMEM((rows, block), bf16),
            pltpu.VMEM((breadth, basis), bf16),
            pltpu.VMEM((3 * part, breadth), bf16),
        ],
        compiler_params=params,
        name="first_layer",
    )(
        edge_count,
        species_row,
        halo_species,
        inner_edges,
        outer_edges,
        inner_vec,
        outer_vec,
        embed,
        mix_in,
        radial_turned,
        radial_mid,
        radial_out,
    )
    state, scalars, table, halo_table, inner_hidden, outer_hidden = pl.pallas_call(
        functools.partial(middle_kernel, slabs, parts, block),
        out_shape=(
            jax.ShapeDtypeStruct((9, chans, atoms), f32),
            jax.ShapeDtypeStruct((chans, atoms), f32),
            jax.ShapeDtypeStruct((rows, atoms), bf16),
            jax.ShapeDtypeStruct((rows, 2 * held), bf16),
            jax.ShapeDtypeStruct((breadth, inner_total), bf16),
            jax.ShapeDtypeStruct((breadth, outer_total), bf16),
        ),
        in_specs=[vmem] * 11,
        out_specs=(vmem, vmem, vmem, vmem, anywhere, anywhere),
        scratch_shapes=[
            pltpu.VMEM((breadth, inner_total), bf16),
            pltpu.VMEM((breadth, outer_total), bf16),
            dma((2,)),
            pltpu.VMEM((parts, rows, atoms), bf16),
            pltpu.VMEM((2, rows, held), bf16),
            pltpu.VMEM((2, rows, held), bf16),
            dma((parts - 1, 9)),
            dma((parts - 1, 9)),
            dma((2,)),
            dma((2,)),
        ],
        compiler_params=remote(1),
        name="middle",
    )(
        species_row,
        halo,
        agg,
        embed,
        mix_in,
        scalar,
        mix_irrep,
        inner_basis,
        outer_basis,
        radial_turned,
        radial_mid,
    )
    agg = pl.pallas_call(
        functools.partial(second_kernel, block),
        out_shape=jax.ShapeDtypeStruct((rows, atoms), bf16),
        in_specs=[smem] + [vmem] * 6 + [anywhere] * 2 + [vmem],
        out_specs=vmem,
        scratch_shapes=[
            pltpu.VMEM((rows, atoms), f32),
            pltpu.VMEM((paths * part, block), f32),
            pltpu.VMEM((rows, block), f32),
            pltpu.VMEM((rows, block), bf16),
            pltpu.VMEM((breadth, inner_total), bf16),
            pltpu.VMEM((breadth, outer_total), bf16),
            dma((inner_total // block,)),
            dma((outer_total // block,)),
        ],
        compiler_params=params,
        name="second_layer",
    )(
        edge_count,
        table,
        halo_table,
        inner_edges,
        outer_edges,
        inner_vec,
        outer_vec,
        inner_hidden,
        outer_hidden,
        radial_out,
    )
    every, atom_energy, mean_energy = pl.pallas_call(
        functools.partial(energy_kernel, slabs, parts),
        out_shape=(
            jax.ShapeDtypeStruct((parts, rows, atoms), bf16),
            jax.ShapeDtypeStruct((1, atoms), f32),
            jax.ShapeDtypeStruct((1, 1), f32),
        ),
        in_specs=[vmem, smem] + [vmem] * 4 + [smem],
        out_specs=(vmem, vmem, vmem),
        scratch_shapes=[
            pltpu.VMEM((parts, rows, atoms), bf16),
            pltpu.VMEM((slabs, 8, 128), f32),
            dma((parts - 1, 9)),
            dma((parts - 1, 9)),
            dma((slabs - 1,)),
            dma((slabs - 1,)),
        ],
        compiler_params=remote(2),
        name="energies",
    )(
        species_row,
        atom_count,
        agg,
        scalars,
        scalar,
        readout[None, :],
        species_energy,
    )
    node_state, atom_energy, mean_energy = pl.pallas_call(
        last_kernel,
        out_shape=(
            jax.ShapeDtypeStruct((9, chans, atoms), f32),
            jax.ShapeDtypeStruct((1, atoms), f32),
            jax.ShapeDtypeStruct((1, 1), f32),
        ),
        in_specs=[vmem] * 6,
        out_specs=(vmem, vmem, vmem),
        compiler_params=params,
        name="last",
    )(every, state, scalar, mix_irrep, atom_energy, mean_energy)
    return (node_state, atom_energy[0], mean_energy[0, 0])


def solution(mesh):
    return jax.shard_map(
        local,
        mesh=mesh,
        in_specs=(
            P("slab"),
            P("slab"),
            P("slab", None, None),
            P("slab", None),
            P(None, "slab"),
            P(None, "slab"),
            P(None, "slab"),
            P(None, "slab"),
            P(),
            P(),
            P(),
            P(None, None, "chan", None),
            P(None, None, "chan", None),
            P(),
            P(),
            P(),
            P(),
        ),
        out_specs=(P(None, None, "slab"), P("slab"), P()),
        check_vma=False,
    )
```

```python
import functools
import math

import jax
import jax.numpy as jnp
from jax import lax
from jax.experimental import pallas as pl
from jax.experimental.pallas import tpu as pltpu
from jax.sharding import PartitionSpec as P

cutoff = 5.0
neighbour_norm = 1.0 / math.sqrt(48.0)
root_three = math.sqrt(3.0)
half_root = 0.5 * math.sqrt(3.0)
BLOCK = 2048
WIDE = 4096
f32 = jnp.float32
bf16 = jnp.bfloat16


def dot(a, b):
    return jnp.dot(a, b, preferred_element_type=f32)


def dot_nt(a, b):
    return lax.dot_general(a, b, (((1,), (1,)), ((), ())), preferred_element_type=f32)


def sigmoid(v):
    return 0.5 * jnp.tanh(0.5 * v) + 0.5


def silu(v):
    half = 0.5 * v
    return half * jnp.tanh(half) + half


def onehot_rows(index, rows):
    slots = lax.broadcasted_iota(jnp.int32, (rows, index.shape[1]), 0)
    return jnp.where(slots == index, 1.0, 0.0).astype(bf16)


def turned(matrix):
    return matrix.astype(f32).T.astype(bf16)


def initial(embed_ref, species_row):
    return dot(turned(embed_ref[...]), onehot_rows(species_row, embed_ref.shape[0]))


def unit(vec):
    x, y, z = vec[0:1], vec[1:2], vec[2:3]
    squared = x * x + y * y + z * z
    inverse = lax.rsqrt(squared + 0.25)
    return squared, inverse, x * inverse, y * inverse, z * inverse


def bessel_rows(squared, inverse, orders):
    length = jnp.sqrt(squared)
    fraction = jnp.minimum(length * (1.0 / cutoff), 1.0)
    cube = fraction * fraction * fraction
    sixth = cube * cube
    envelope = 1.0 - sixth * (28.0 - fraction * (48.0 - 21.0 * fraction))
    half = length * (0.5 * math.pi / cutoff)
    h2 = half * half
    sine = 1.0
    cosine = 1.0
    for order in range(12, 0, -2):
        sine = 1.0 - sine * h2 * (1.0 / ((order + 1) * order))
        cosine = 1.0 - cosine * h2 * (1.0 / (order * (order - 1)))
    sine = sine * half
    twice_cos = 2.0 - 4.0 * sine * sine
    first = 2.0 * sine * cosine
    scale = math.sqrt(2.0 / cutoff) * inverse * envelope
    before, now = jnp.zeros_like(first), first * scale
    rows = []
    for _ in range(orders):
        rows.append(now)
        before, now = now, twice_cos * now - before
    return jnp.concatenate(rows, axis=0)


def harmonics(x, y, z):
    return [
        root_three * x * y,
        root_three * y * z,
        0.5 * (2.0 * z * z - x * x - y * y),
        root_three * x * z,
        half_root * (x * x - y * y),
    ]


def radial(entry, mid, basis):
    hidden = silu(dot(entry, basis)).astype(bf16)
    return silu(dot(mid, hidden)).astype(bf16)


def first_kernel(
    block,
    count_ref,
    species_ref,
    halo_species_ref,
    inner_edges_ref,
    outer_edges_ref,
    inner_vec_ref,
    outer_vec_ref,
    embed_ref,
    mix_ref,
    radial_in_ref,
    radial_mid_ref,
    radial_out_ref,
    agg_ref,
    inner_basis_ref,
    outer_basis_ref,
    acc_ref,
    table_ref,
    mess_ref,
    entry_ref,
    paths_ref,
):
    chans = mix_ref.shape[2]
    atoms = species_ref.shape[1]
    for slot, ref in enumerate((species_ref, halo_species_ref)):
        init = initial(embed_ref, ref[...]).astype(bf16)
        table_ref[slot] = dot(mix_ref[0, 0], init).astype(bf16)
    acc_ref[...] = jnp.zeros_like(acc_ref)
    entry_ref[...] = turned(radial_in_ref[0])
    for k, path in enumerate((0, 3, 7)):
        paths_ref[k * chans : (k + 1) * chans] = radial_out_ref[0, path]

    def visit(slot, edges_ref, vec_ref, basis_ref, live, step):
        offset = pl.multiple_of(step * block, block)
        span = pl.ds(offset, block)
        source = onehot_rows(edges_ref[0:1, span], table_ref.shape[2])
        gathered = dot(table_ref[slot], source)
        squared, inverse, x, y, z = unit(vec_ref[:, span])
        basis = bessel_rows(squared, inverse, radial_in_ref.shape[1]).astype(bf16)
        basis_ref[:, span] = basis
        weights = dot(paths_ref[...], radial(entry_ref[...], radial_mid_ref[0], basis))
        q = harmonics(x, y, z)
        lanes = lax.broadcasted_iota(jnp.int32, (1, block), 1) + offset
        target = jnp.where(lanes < live, edges_ref[1:2, span], -1)
        by_vector = weights[chans : 2 * chans] * gathered
        by_tensor = weights[2 * chans : 3 * chans] * gathered
        mess_ref[0:chans] = (weights[0:chans] * gathered).astype(bf16)
        for k, part in enumerate((x, y, z)):
            mess_ref[(1 + k) * chans : (2 + k) * chans] = (by_vector * part).astype(bf16)
        for k, part in enumerate(q):
            mess_ref[(4 + k) * chans : (5 + k) * chans] = (by_tensor * part).astype(bf16)
        acc_ref[...] += dot_nt(mess_ref[...], onehot_rows(target, atoms))

    def run(slot, edges_ref, vec_ref, basis_ref, live):
        def body(step, carry):
            visit(slot, edges_ref, vec_ref, basis_ref, live, step)
            return carry

        lax.fori_loop(0, lax.div(live + (block - 1), block), body, 0)

    run(0, inner_edges_ref, inner_vec_ref, inner_basis_ref, count_ref[0, 0])
    run(1, outer_edges_ref, outer_vec_ref, outer_basis_ref, count_ref[0, 1])
    agg_ref[...] = (acc_ref[...] * neighbour_norm).astype(bf16)


def second_kernel(
    block,
    count_ref,
    table_ref,
    halo_table_ref,
    inner_edges_ref,
    outer_edges_ref,
    inner_vec_ref,
    outer_vec_ref,
    inner_hidden_ref,
    outer_hidden_ref,
    radial_out_ref,
    out_ref,
    acc_ref,
    weight_ref,
    source_ref,
    mess_ref,
    inner_held_ref,
    outer_held_ref,
    inner_sem,
    outer_sem,
):
    chans = table_ref.shape[0] // 9
    atoms = out_ref.shape[1]
    lists = (
        (inner_hidden_ref, inner_held_ref, inner_sem, count_ref[0, 0]),
        (outer_hidden_ref, outer_held_ref, outer_sem, count_ref[0, 1]),
    )

    def fetch(hidden_ref, held_ref, sem, step):
        span = pl.ds(pl.multiple_of(step * block, block), block)
        return pltpu.make_async_copy(hidden_ref.at[:, span], held_ref.at[:, span], sem.at[step])

    for hidden_ref, held_ref, sem, live in lists:

        def begin(step, carry, hidden_ref=hidden_ref, held_ref=held_ref, sem=sem):
            fetch(hidden_ref, held_ref, sem, step).start()
            return carry

        lax.fori_loop(0, lax.div(live + (block - 1), block), begin, 0)
    acc_ref[...] = jnp.zeros_like(acc_ref)
    paths, _, breadth = radial_out_ref.shape[1:]
    radial = radial_out_ref[1].reshape(paths * chans, breadth)

    def visit(table_ref, edges_ref, vec_ref, held, step):
        hidden_ref, held_ref, sem, live = held
        fetch(hidden_ref, held_ref, sem, step).wait()
        offset = pl.multiple_of(step * block, block)
        span = pl.ds(offset, block)
        onehot = onehot_rows(edges_ref[0:1, span], table_ref.shape[1])
        source_ref[...] = dot(table_ref[...], onehot)
        weight_ref[...] = dot(radial, held_ref[:, span])
        _, _, x_row, y_row, z_row = unit(vec_ref[:, span])
        q_rows = harmonics(x_row, y_row, z_row)
        height, width = 16, 128
        for lane in range(0, block, width):
            cols = slice(lane, lane + width)

            def wide(row):
                return jnp.broadcast_to(row[:, cols], (height, width))

            x, y, z = wide(x_row), wide(y_row), wide(z_row)
            q = [wide(row) for row in q_rows]
            hx, hy, hz = half_root * x, half_root * y, half_root * z
            for low in range(0, chans, height):

                def at(ref, k):
                    return ref[k * chans + low : k * chans + low + height, cols]

                def put(k, value):
                    mess_ref[k * chans + low : k * chans + low + height, cols] = value.astype(bf16)

                s = at(source_ref, 0)
                v = [at(source_ref, k) for k in (1, 2, 3)]
                t = [at(source_ref, k) for k in (4, 5, 6, 7, 8)]
                along = v[0] * x + v[1] * y + v[2] * z
                tq = t[0] * q[0] + t[1] * q[1] + t[2] * q[2] + t[3] * q[3] + t[4] * q[4]
                put(0, at(weight_ref, 0) * s + at(weight_ref, 1) * tq + at(weight_ref, 2) * along)
                ws = at(weight_ref, 3) * s
                w4, w5, w6 = at(weight_ref, 4), at(weight_ref, 5), at(weight_ref, 6)
                cross = [
                    v[1] * z - v[2] * y,
                    v[2] * x - v[0] * z,
                    v[0] * y - v[1] * x,
                ]
                t3 = 0.5 * t[2]
                grad = [
                    hy * t[0] - x * t3 + hz * t[3] + hx * t[4],
                    hx * t[0] + hz * t[1] - y * t3 - hy * t[4],
                    hy * t[1] + z * t[2] + hx * t[3],
                ]
                for k, part in enumerate((x, y, z)):
                    put(1 + k, ws * part + w4 * v[k] + w5 * cross[k] + w6 * grad[k])
                ws = at(weight_ref, 7) * s
                w8, w9 = at(weight_ref, 8), at(weight_ref, 9)
                sym = [
                    hy * v[0] + hx * v[1],
                    hz * v[1] + hy * v[2],
                    1.5 * v[2] * z - 0.5 * along,
                    hz * v[0] + hx * v[2],
                    hx * v[0] - hy * v[1],
                ]
                for k in range(5):
                    put(4 + k, ws * q[k] + w8 * t[k] + w9 * sym[k])
        lanes = lax.broadcasted_iota(jnp.int32, (1, block), 1) + offset
        target = jnp.where(lanes < live, edges_ref[1:2, span], -1)
        acc_ref[...] += dot_nt(mess_ref[...], onehot_rows(target, atoms))

    def run(table, edges_ref, vec_ref, held):
        def body(step, carry):
            visit(table, edges_ref, vec_ref, held, step)
            return carry

        lax.fori_loop(0, lax.div(held[3] + (block - 1), block), body, 0)

    run(table_ref, inner_edges_ref, inner_vec_ref, lists[0])
    run(halo_table_ref, outer_edges_ref, outer_vec_ref, lists[1])
    out_ref[...] = (acc_ref[...] * neighbour_norm).astype(bf16)


mesh_ids = pl.DeviceIdType.MESH


def greet(peers):
    barrier = pltpu.get_barrier_semaphore()
    for peer in peers:
        pl.semaphore_signal(barrier, inc=1, device_id=peer, device_id_type=mesh_ids)
    pl.semaphore_wait(barrier, len(peers))


def others(axis, total):
    me = lax.axis_index(axis)
    return [{axis: lax.rem(me + step, total)} for step in range(1, total)]


def beside(total):
    me = lax.axis_index("slab")
    return {"slab": lax.rem(me + total - 1, total)}, {"slab": lax.rem(me + 1, total)}


def send_halo(send_ref, land_ref, send_sem, recv_sem, total):
    copies = []
    for side, peer in enumerate(beside(total)):
        copies.append(
            pltpu.make_async_remote_copy(
                src_ref=send_ref.at[side],
                dst_ref=land_ref.at[1 - side],
                send_sem=send_sem.at[side],
                recv_sem=recv_sem.at[side],
                device_id=peer,
                device_id_type=mesh_ids,
            )
        )
    for copy in copies:
        copy.start()
    return copies


def species_kernel(slabs, species_ref, halo_ref, out_ref, send_ref, land_ref, send_sem, recv_sem):
    values = jnp.broadcast_to(species_ref[...].astype(f32), (16, species_ref.shape[1])).astype(bf16)
    for side in range(2):
        onehot = onehot_rows(halo_ref[side : side + 1], species_ref.shape[1])
        send_ref[side] = dot(values, onehot)[0:8]
    greet(beside(slabs))
    for copy in send_halo(send_ref, land_ref, send_sem, recv_sem, slabs):
        copy.wait()
    out_ref[...] = jnp.concatenate([land_ref[0, 0:1], land_ref[1, 0:1]], axis=1).astype(jnp.int32)


def exchange(agg_ref, all_ref, send_sem, recv_sem, total):
    part = agg_ref.shape[0] // 9
    me = lax.axis_index("chan")
    peers = others("chan", total)
    copies = []
    for k in range(9):
        span = slice(k * part, (k + 1) * part)
        for i, peer in enumerate(peers):
            copies.append(
                pltpu.make_async_remote_copy(
                    src_ref=agg_ref.at[span],
                    dst_ref=all_ref.at[me, span],
                    send_sem=send_sem.at[i, k],
                    recv_sem=recv_sem.at[i, k],
                    device_id=peer,
                    device_id_type=mesh_ids,
                )
            )
    for copy in copies:
        copy.start()
    all_ref[me] = agg_ref[...]

    def component(k):
        for copy in copies[k * len(peers) : (k + 1) * len(peers)]:
            copy.wait_recv()
        span = slice(k * part, (k + 1) * part)
        return jnp.concatenate([all_ref[i, span] for i in range(total)], axis=0)

    return copies, component


class Updates:
    def __init__(self, component, layer, scalar_ref, irrep_ref):
        self.component, self.layer, self.irrep = component, layer, irrep_ref
        chans = irrep_ref.shape[2]
        y = dot(turned(scalar_ref[layer]), component(0))
        self.scalar = silu(y[:chans])
        self.gates = sigmoid(y[chans : 2 * chans]), sigmoid(y[2 * chans :])

    def __getitem__(self, k):
        if k == 0:
            return self.scalar
        kind = 0 if k < 4 else 1
        return self.gates[kind] * dot(self.irrep[self.layer, kind], self.component(k))


def middle_kernel(
    slabs,
    parts,
    block,
    species_ref,
    halo_ref,
    agg_ref,
    embed_ref,
    mix_ref,
    scalar_ref,
    irrep_ref,
    inner_basis_ref,
    outer_basis_ref,
    radial_in_ref,
    radial_mid_ref,
    state_ref,
    scalars_ref,
    table_ref,
    halo_table_ref,
    inner_hidden_ref,
    outer_hidden_ref,
    inner_held_ref,
    outer_held_ref,
    out_sem,
    all_ref,
    send_ref,
    land_ref,
    agg_send,
    agg_recv,
    halo_send,
    halo_recv,
):
    part = mix_ref.shape[2]
    greet(others("chan", parts) + list(beside(slabs)))
    copies, component = exchange(agg_ref, all_ref, agg_send, agg_recv, parts)
    entry = turned(radial_in_ref[1])
    writes = []
    lists = (
        (inner_basis_ref, inner_held_ref, inner_hidden_ref),
        (outer_basis_ref, outer_held_ref, outer_hidden_ref),
    )
    for i, (basis_ref, held_ref, hidden_ref) in enumerate(lists):

        def body(step, carry, basis_ref=basis_ref, held_ref=held_ref):
            span = pl.ds(pl.multiple_of(step * block, block), block)
            held_ref[:, span] = radial(entry, radial_mid_ref[1], basis_ref[:, span])
            return carry

        lax.fori_loop(0, basis_ref.shape[1] // block, body, 0)
        writes.append(pltpu.make_async_copy(held_ref, hidden_ref, out_sem.at[i]))
    onehots = jnp.concatenate(
        [onehot_rows(halo_ref[side : side + 1], table_ref.shape[1]) for side in range(2)], axis=1
    )
    start = initial(embed_ref, species_ref[...])
    outs = Updates(component, 0, scalar_ref, irrep_ref)
    held = halo_ref.shape[1]
    for k in range(9):
        out = outs[k]
        if k == 0:
            for write in writes:
                write.start()
            out += start
            scalars_ref[...] = out
        state_ref[k] = out
        which = 0 if k == 0 else (1 if k < 4 else 2)
        span = slice(k * part, (k + 1) * part)
        mixed = dot(mix_ref[1, which], out.astype(bf16)).astype(bf16)
        table_ref[span] = mixed
        picked = dot(mixed, onehots).astype(bf16)
        for side in range(2):
            send_ref[side, span] = picked[:, side * held : (side + 1) * held]
    for copy in copies:
        copy.wait_send()
    for copy in send_halo(send_ref, land_ref, halo_send, halo_recv, slabs):
        copy.wait()
    for write in writes:
        write.wait()
    for side in range(2):
        halo_table_ref[:, side * held : (side + 1) * held] = land_ref[side]


def energy_kernel(
    slabs,
    parts,
    species_ref,
    count_ref,
    agg_ref,
    scalars_ref,
    scalar_ref,
    readout_ref,
    energy_ref,
    every_ref,
    atom_ref,
    mean_ref,
    all_ref,
    energies_ref,
    agg_send,
    agg_recv,
    energy_send,
    energy_recv,
):
    peers = others("slab", slabs)
    greet(others("chan", parts) + peers)
    copies, component = exchange(agg_ref, all_ref, agg_send, agg_recv, parts)
    chans, atoms = scalars_ref.shape
    lines = lax.broadcasted_iota(jnp.int32, (chans, chans), 0)
    across = lax.broadcasted_iota(jnp.int32, (chans, chans), 1)
    readout = jnp.sum(jnp.where(lines == across, readout_ref[...], 0.0), axis=1, keepdims=True)
    own = jnp.zeros((1, atoms), f32)
    for kind in range(energy_ref.shape[0]):
        own = jnp.where(species_ref[...] == kind, energy_ref[kind], own)
    lanes = lax.broadcasted_iota(jnp.int32, (1, atoms), 1)
    weight = turned(scalar_ref[1])[:chans]
    out = scalars_ref[...] + silu(dot(weight, component(0)))
    total = jnp.sum(out * readout, axis=0, keepdims=True) + own
    total = jnp.where(lanes < count_ref[0], total, 0.0)
    me = lax.axis_index("slab")
    energies_ref[me] = jnp.broadcast_to(
        jnp.sum(total, axis=1, keepdims=True), energies_ref.shape[1:]
    )
    atom_ref[...] = total
    part = agg_ref.shape[0] // 9
    every_ref[:, :part] = all_ref[:, :part]
    sums = [
        pltpu.make_async_remote_copy(
            src_ref=energies_ref.at[me],
            dst_ref=energies_ref.at[me],
            send_sem=energy_send.at[i],
            recv_sem=energy_recv.at[i],
            device_id=peer,
            device_id_type=mesh_ids,
        )
        for i, peer in enumerate(peers)
    ]
    for copy in sums:
        copy.start()
    for k in range(1, 9):
        component(k)
    every_ref[:, part:] = all_ref[:, part:]
    for copy in copies:
        copy.wait_send()
    for copy in sums:
        copy.wait()
    mean_ref[...] = jnp.sum(energies_ref[...], axis=0)[0:1, 0:1] * (1.0 / (atoms * slabs))


def last_kernel(
    every_ref, state_in_ref, scalar_ref, irrep_ref, atom_in_ref, mean_in_ref, state_ref, atom_ref, mean_ref
):
    part = every_ref.shape[1] // 9

    def component(k):
        span = slice(k * part, (k + 1) * part)
        return jnp.concatenate([every_ref[i, span] for i in range(every_ref.shape[0])], axis=0)

    outs = Updates(component, 1, scalar_ref, irrep_ref)
    for k in range(9):
        state_ref[k] = state_in_ref[k] + outs[k]
    atom_ref[...] = atom_in_ref[...]
    mean_ref[...] = mean_in_ref[...]


vmem = pl.BlockSpec(memory_space=pltpu.VMEM)
anywhere = pl.BlockSpec(memory_space=pl.ANY)
smem = pl.BlockSpec(memory_space=pltpu.SMEM)
params = pltpu.CompilerParams(vmem_limit_bytes=56 * 1024 * 1024)


def remote(number):
    return pltpu.CompilerParams(
        vmem_limit_bytes=56 * 1024 * 1024, collective_id=number, has_side_effects=True
    )


def local(
    species,
    atom_count,
    halo_index,
    edge_count,
    inner_edges,
    outer_edges,
    inner_vec,
    outer_vec,
    embed_table,
    radial_in,
    radial_mid,
    radial_out,
    mix_in,
    mix_scalar,
    mix_irrep,
    readout,
    species_energy,
):
    slabs = lax.axis_size("slab")
    parts = lax.axis_size("chan")
    atoms = species.shape[0]
    chans = embed_table.shape[0]
    part = mix_in.shape[2]
    breadth = radial_mid.shape[1]
    basis = radial_in.shape[2]
    paths = radial_out.shape[1]
    halo = halo_index[0]
    held = halo.shape[1]
    rows = 9 * part
    dma = pltpu.SemaphoreType.DMA
    species_row = species[None, :]
    embed = embed_table.T
    scalar = jnp.swapaxes(mix_scalar, 1, 2)
    halo_species = pl.pallas_call(
        functools.partial(species_kernel, slabs),
        out_shape=jax.ShapeDtypeStruct((1, 2 * held), jnp.int32),
        in_specs=[vmem] * 2,
        out_specs=vmem,
        scratch_shapes=[
            pltpu.VMEM((2, 8, held), f32),
            pltpu.VMEM((2, 8, held), f32),
            dma((2,)),
            dma((2,)),
        ],
        compiler_params=remote(0),
        name="halo_species",
    )(species_row, halo)
    block = math.gcd(BLOCK, math.gcd(inner_edges.shape[1], outer_edges.shape[1]))
    inner_total, outer_total = inner_edges.shape[1], outer_edges.shape[1]
    radial_turned = jnp.swapaxes(radial_in, 1, 2)
    agg, inner_basis, outer_basis = pl.pallas_call(
        functools.partial(first_kernel, block),
        out_shape=(
            jax.ShapeDtypeStruct((rows, atoms), bf16),
            jax.ShapeDtypeStruct((basis, inner_total), bf16),
            jax.ShapeDtypeStruct((basis, outer_total), bf16),
        ),
        in_specs=[smem] + [vmem] * 11,
        out_specs=(vmem, vmem, vmem),
        scratch_shapes=[
            pltpu.VMEM((rows, atoms), f32),
            pltpu.VMEM((2, part, atoms), bf16),
            pltpu.VMEM((rows, block), bf16),
            pltpu.VMEM((breadth, basis), bf16),
            pltpu.VMEM((3 * part, breadth), bf16),
        ],
        compiler_params=params,
        name="first_layer",
    )(
        edge_count,
        species_row,
        halo_species,
        inner_edges,
        outer_edges,
        inner_vec,
        outer_vec,
        embed,
        mix_in,
        radial_turned,
        radial_mid,
        radial_out,
    )
    state, scalars, table, halo_table, inner_hidden, outer_hidden = pl.pallas_call(
        functools.partial(
            middle_kernel, slabs, parts, math.gcd(WIDE, math.gcd(inner_total, outer_total))
        ),
        out_shape=(
            jax.ShapeDtypeStruct((9, chans, atoms), f32),
            jax.ShapeDtypeStruct((chans, atoms), f32),
            jax.ShapeDtypeStruct((rows, atoms), bf16),
            jax.ShapeDtypeStruct((rows, 2 * held), bf16),
            jax.ShapeDtypeStruct((breadth, inner_total), bf16),
            jax.ShapeDtypeStruct((breadth, outer_total), bf16),
        ),
        in_specs=[vmem] * 11,
        out_specs=(vmem, vmem, vmem, vmem, anywhere, anywhere),
        scratch_shapes=[
            pltpu.VMEM((breadth, inner_total), bf16),
            pltpu.VMEM((breadth, outer_total), bf16),
            dma((2,)),
            pltpu.VMEM((parts, rows, atoms), bf16),
            pltpu.VMEM((2, rows, held), bf16),
            pltpu.VMEM((2, rows, held), bf16),
            dma((parts - 1, 9)),
            dma((parts - 1, 9)),
            dma((2,)),
            dma((2,)),
        ],
        compiler_params=remote(1),
        name="middle",
    )(
        species_row,
        halo,
        agg,
        embed,
        mix_in,
        scalar,
        mix_irrep,
        inner_basis,
        outer_basis,
        radial_turned,
        radial_mid,
    )
    agg = pl.pallas_call(
        functools.partial(second_kernel, block),
        out_shape=jax.ShapeDtypeStruct((rows, atoms), bf16),
        in_specs=[smem] + [vmem] * 6 + [anywhere] * 2 + [vmem],
        out_specs=vmem,
        scratch_shapes=[
            pltpu.VMEM((rows, atoms), f32),
            pltpu.VMEM((paths * part, block), f32),
            pltpu.VMEM((rows, block), f32),
            pltpu.VMEM((rows, block), bf16),
            pltpu.VMEM((breadth, inner_total), bf16),
            pltpu.VMEM((breadth, outer_total), bf16),
            dma((inner_total // block,)),
            dma((outer_total // block,)),
        ],
        compiler_params=params,
        name="second_layer",
    )(
        edge_count,
        table,
        halo_table,
        inner_edges,
        outer_edges,
        inner_vec,
        outer_vec,
        inner_hidden,
        outer_hidden,
        radial_out,
    )
    every, atom_energy, mean_energy = pl.pallas_call(
        functools.partial(energy_kernel, slabs, parts),
        out_shape=(
            jax.ShapeDtypeStruct((parts, rows, atoms), bf16),
            jax.ShapeDtypeStruct((1, atoms), f32),
            jax.ShapeDtypeStruct((1, 1), f32),
        ),
        in_specs=[vmem, smem] + [vmem] * 4 + [smem],
        out_specs=(vmem, vmem, vmem),
        scratch_shapes=[
            pltpu.VMEM((parts, rows, atoms), bf16),
            pltpu.VMEM((slabs, 8, 128), f32),
            dma((parts - 1, 9)),
            dma((parts - 1, 9)),
            dma((slabs - 1,)),
            dma((slabs - 1,)),
        ],
        compiler_params=remote(2),
        name="energies",
    )(
        species_row,
        atom_count,
        agg,
        scalars,
        scalar,
        readout[None, :],
        species_energy,
    )
    node_state, atom_energy, mean_energy = pl.pallas_call(
        last_kernel,
        out_shape=(
            jax.ShapeDtypeStruct((9, chans, atoms), f32),
            jax.ShapeDtypeStruct((1, atoms), f32),
            jax.ShapeDtypeStruct((1, 1), f32),
        ),
        in_specs=[vmem] * 6,
        out_specs=(vmem, vmem, vmem),
        compiler_params=params,
        name="last",
    )(every, state, scalar, mix_irrep, atom_energy, mean_energy)
    return (node_state, atom_energy[0], mean_energy[0, 0])


def solution(mesh):
    return jax.shard_map(
        local,
        mesh=mesh,
        in_specs=(
            P("slab"),
            P("slab"),
            P("slab", None, None),
            P("slab", None),
            P(None, "slab"),
            P(None, "slab"),
            P(None, "slab"),
            P(None, "slab"),
            P(),
            P(),
            P(),
            P(None, None, "chan", None),
            P(None, None, "chan", None),
            P(),
            P(),
            P(),
            P(),
        ),
        out_specs=(P(None, None, "slab"), P("slab"), P()),
        check_vma=False,
    )
```

```python
import functools
import math

import jax
import jax.numpy as jnp
from jax import lax
from jax.experimental import pallas as pl
from jax.experimental.pallas import tpu as pltpu
from jax.sharding import PartitionSpec as P

cutoff = 5.0
neighbour_norm = 1.0 / math.sqrt(48.0)
root_three = math.sqrt(3.0)
half_root = 0.5 * math.sqrt(3.0)
BLOCK = 2048
WIDE = 4096
GROUPS = ((0, 1), (1, 4), (4, 9))
f32 = jnp.float32
bf16 = jnp.bfloat16


def dot(a, b):
    return jnp.dot(a, b, preferred_element_type=f32)


def dot_nt(a, b):
    return lax.dot_general(a, b, (((1,), (1,)), ((), ())), preferred_element_type=f32)


def sigmoid(v):
    return 0.5 * jnp.tanh(0.5 * v) + 0.5


def silu(v):
    half = 0.5 * v
    return half * jnp.tanh(half) + half


def onehot_rows(index, rows):
    slots = lax.broadcasted_iota(jnp.int32, (rows, index.shape[1]), 0)
    return jnp.where(slots == index, 1.0, 0.0).astype(bf16)


def turned(matrix):
    return matrix.astype(f32).T.astype(bf16)


def initial(embed_ref, species_row):
    return dot(turned(embed_ref[...]), onehot_rows(species_row, embed_ref.shape[0]))


def unit(vec):
    x, y, z = vec[0:1], vec[1:2], vec[2:3]
    squared = x * x + y * y + z * z
    inverse = lax.rsqrt(squared + 0.25)
    return squared, inverse, x * inverse, y * inverse, z * inverse


def bessel_rows(squared, inverse, orders):
    length = jnp.sqrt(squared)
    fraction = jnp.minimum(length * (1.0 / cutoff), 1.0)
    cube = fraction * fraction * fraction
    sixth = cube * cube
    envelope = 1.0 - sixth * (28.0 - fraction * (48.0 - 21.0 * fraction))
    half = length * (0.5 * math.pi / cutoff)
    h2 = half * half
    sine = 1.0
    cosine = 1.0
    for order in range(12, 0, -2):
        sine = 1.0 - sine * h2 * (1.0 / ((order + 1) * order))
        cosine = 1.0 - cosine * h2 * (1.0 / (order * (order - 1)))
    sine = sine * half
    twice_cos = 2.0 - 4.0 * sine * sine
    first = 2.0 * sine * cosine
    scale = math.sqrt(2.0 / cutoff) * inverse * envelope
    before, now = jnp.zeros_like(first), first * scale
    rows = []
    for _ in range(orders):
        rows.append(now)
        before, now = now, twice_cos * now - before
    return jnp.concatenate(rows, axis=0)


def harmonics(x, y, z):
    return [
        root_three * x * y,
        root_three * y * z,
        0.5 * (2.0 * z * z - x * x - y * y),
        root_three * x * z,
        half_root * (x * x - y * y),
    ]


def radial(entry, mid, basis):
    hidden = silu(dot(entry, basis)).astype(bf16)
    return silu(dot(mid, hidden)).astype(bf16)


def first_kernel(
    block,
    count_ref,
    species_ref,
    halo_species_ref,
    inner_edges_ref,
    outer_edges_ref,
    inner_vec_ref,
    outer_vec_ref,
    embed_ref,
    mix_ref,
    radial_in_ref,
    radial_mid_ref,
    radial_out_ref,
    agg_ref,
    inner_basis_ref,
    outer_basis_ref,
    acc_ref,
    table_ref,
    mess_ref,
    entry_ref,
    paths_ref,
):
    chans = mix_ref.shape[2]
    atoms = species_ref.shape[1]
    for slot, ref in enumerate((species_ref, halo_species_ref)):
        init = initial(embed_ref, ref[...]).astype(bf16)
        table_ref[slot] = dot(mix_ref[0, 0], init).astype(bf16)
    acc_ref[...] = jnp.zeros_like(acc_ref)
    entry_ref[...] = turned(radial_in_ref[0])
    for k, path in enumerate((0, 3, 7)):
        paths_ref[k * chans : (k + 1) * chans] = radial_out_ref[0, path]

    def visit(slot, edges_ref, vec_ref, basis_ref, live, step):
        offset = pl.multiple_of(step * block, block)
        span = pl.ds(offset, block)
        source = onehot_rows(edges_ref[0:1, span], table_ref.shape[2])
        gathered = dot(table_ref[slot], source)
        squared, inverse, x, y, z = unit(vec_ref[:, span])
        basis = bessel_rows(squared, inverse, radial_in_ref.shape[1]).astype(bf16)
        basis_ref[:, span] = basis
        weights = dot(paths_ref[...], radial(entry_ref[...], radial_mid_ref[0], basis))
        q = harmonics(x, y, z)
        lanes = lax.broadcasted_iota(jnp.int32, (1, block), 1) + offset
        target = jnp.where(lanes < live, edges_ref[1:2, span], -1)
        by_vector = weights[chans : 2 * chans] * gathered
        by_tensor = weights[2 * chans : 3 * chans] * gathered
        mess_ref[0:chans] = (weights[0:chans] * gathered).astype(bf16)
        for k, part in enumerate((x, y, z)):
            mess_ref[(1 + k) * chans : (2 + k) * chans] = (by_vector * part).astype(bf16)
        for k, part in enumerate(q):
            mess_ref[(4 + k) * chans : (5 + k) * chans] = (by_tensor * part).astype(bf16)
        acc_ref[...] += dot_nt(mess_ref[...], onehot_rows(target, atoms))

    def run(slot, edges_ref, vec_ref, basis_ref, live):
        def body(step, carry):
            visit(slot, edges_ref, vec_ref, basis_ref, live, step)
            return carry

        lax.fori_loop(0, lax.div(live + (block - 1), block), body, 0)

    run(0, inner_edges_ref, inner_vec_ref, inner_basis_ref, count_ref[0, 0])
    run(1, outer_edges_ref, outer_vec_ref, outer_basis_ref, count_ref[0, 1])
    agg_ref[...] = (acc_ref[...] * neighbour_norm).astype(bf16)


def second_kernel(
    block,
    count_ref,
    table_ref,
    halo_table_ref,
    inner_edges_ref,
    outer_edges_ref,
    inner_vec_ref,
    outer_vec_ref,
    inner_hidden_ref,
    outer_hidden_ref,
    radial_out_ref,
    out_ref,
    acc_ref,
    weight_ref,
    source_ref,
    mess_ref,
    inner_held_ref,
    outer_held_ref,
    inner_sem,
    outer_sem,
):
    chans = table_ref.shape[0] // 9
    atoms = out_ref.shape[1]
    lists = (
        (inner_hidden_ref, inner_held_ref, inner_sem, count_ref[0, 0]),
        (outer_hidden_ref, outer_held_ref, outer_sem, count_ref[0, 1]),
    )

    def fetch(hidden_ref, held_ref, sem, step):
        span = pl.ds(pl.multiple_of(step * block, block), block)
        return pltpu.make_async_copy(hidden_ref.at[:, span], held_ref.at[:, span], sem.at[step])

    for hidden_ref, held_ref, sem, live in lists:

        def begin(step, carry, hidden_ref=hidden_ref, held_ref=held_ref, sem=sem):
            fetch(hidden_ref, held_ref, sem, step).start()
            return carry

        lax.fori_loop(0, lax.div(live + (block - 1), block), begin, 0)
    acc_ref[...] = jnp.zeros_like(acc_ref)
    paths, _, breadth = radial_out_ref.shape[1:]
    radial = radial_out_ref[1].reshape(paths * chans, breadth)

    def visit(table_ref, edges_ref, vec_ref, held, step):
        hidden_ref, held_ref, sem, live = held
        fetch(hidden_ref, held_ref, sem, step).wait()
        offset = pl.multiple_of(step * block, block)
        span = pl.ds(offset, block)
        onehot = onehot_rows(edges_ref[0:1, span], table_ref.shape[1])
        source_ref[...] = dot(table_ref[...], onehot)
        weight_ref[...] = dot(radial, held_ref[:, span])
        _, _, x_row, y_row, z_row = unit(vec_ref[:, span])
        q_rows = harmonics(x_row, y_row, z_row)
        height, width = 16, 128
        for lane in range(0, block, width):
            cols = slice(lane, lane + width)

            def wide(row):
                return jnp.broadcast_to(row[:, cols], (height, width))

            x, y, z = wide(x_row), wide(y_row), wide(z_row)
            q = [wide(row) for row in q_rows]
            hx, hy, hz = half_root * x, half_root * y, half_root * z
            for low in range(0, chans, height):

                def at(ref, k):
                    return ref[k * chans + low : k * chans + low + height, cols]

                def put(k, value):
                    mess_ref[k * chans + low : k * chans + low + height, cols] = value.astype(bf16)

                s = at(source_ref, 0)
                v = [at(source_ref, k) for k in (1, 2, 3)]
                t = [at(source_ref, k) for k in (4, 5, 6, 7, 8)]
                along = v[0] * x + v[1] * y + v[2] * z
                tq = t[0] * q[0] + t[1] * q[1] + t[2] * q[2] + t[3] * q[3] + t[4] * q[4]
                put(0, at(weight_ref, 0) * s + at(weight_ref, 1) * tq + at(weight_ref, 2) * along)
                ws = at(weight_ref, 3) * s
                w4, w5, w6 = at(weight_ref, 4), at(weight_ref, 5), at(weight_ref, 6)
                cross = [
                    v[1] * z - v[2] * y,
                    v[2] * x - v[0] * z,
                    v[0] * y - v[1] * x,
                ]
                t3 = 0.5 * t[2]
                grad = [
                    hy * t[0] - x * t3 + hz * t[3] + hx * t[4],
                    hx * t[0] + hz * t[1] - y * t3 - hy * t[4],
                    hy * t[1] + z * t[2] + hx * t[3],
                ]
                for k, part in enumerate((x, y, z)):
                    put(1 + k, ws * part + w4 * v[k] + w5 * cross[k] + w6 * grad[k])
                ws = at(weight_ref, 7) * s
                w8, w9 = at(weight_ref, 8), at(weight_ref, 9)
                sym = [
                    hy * v[0] + hx * v[1],
                    hz * v[1] + hy * v[2],
                    1.5 * v[2] * z - 0.5 * along,
                    hz * v[0] + hx * v[2],
                    hx * v[0] - hy * v[1],
                ]
                for k in range(5):
                    put(4 + k, ws * q[k] + w8 * t[k] + w9 * sym[k])
        lanes = lax.broadcasted_iota(jnp.int32, (1, block), 1) + offset
        target = jnp.where(lanes < live, edges_ref[1:2, span], -1)
        acc_ref[...] += dot_nt(mess_ref[...], onehot_rows(target, atoms))

    def run(table, edges_ref, vec_ref, held):
        def body(step, carry):
            visit(table, edges_ref, vec_ref, held, step)
            return carry

        lax.fori_loop(0, lax.div(held[3] + (block - 1), block), body, 0)

    run(table_ref, inner_edges_ref, inner_vec_ref, lists[0])
    run(halo_table_ref, outer_edges_ref, outer_vec_ref, lists[1])
    out_ref[...] = (acc_ref[...] * neighbour_norm).astype(bf16)


mesh_ids = pl.DeviceIdType.MESH


def greet(peers):
    barrier = pltpu.get_barrier_semaphore()
    for peer in peers:
        pl.semaphore_signal(barrier, inc=1, device_id=peer, device_id_type=mesh_ids)
    pl.semaphore_wait(barrier, len(peers))


def others(axis, total):
    me = lax.axis_index(axis)
    return [{axis: lax.rem(me + step, total)} for step in range(1, total)]


def beside(total):
    me = lax.axis_index("slab")
    return {"slab": lax.rem(me + total - 1, total)}, {"slab": lax.rem(me + 1, total)}


def send_halo(send_ref, land_ref, send_sem, recv_sem, total):
    copies = []
    for side, peer in enumerate(beside(total)):
        copies.append(
            pltpu.make_async_remote_copy(
                src_ref=send_ref.at[side],
                dst_ref=land_ref.at[1 - side],
                send_sem=send_sem.at[side],
                recv_sem=recv_sem.at[side],
                device_id=peer,
                device_id_type=mesh_ids,
            )
        )
    for copy in copies:
        copy.start()
    return copies


def species_kernel(slabs, species_ref, halo_ref, out_ref, send_ref, land_ref, send_sem, recv_sem):
    values = jnp.broadcast_to(species_ref[...].astype(f32), (16, species_ref.shape[1])).astype(bf16)
    for side in range(2):
        onehot = onehot_rows(halo_ref[side : side + 1], species_ref.shape[1])
        send_ref[side] = dot(values, onehot)[0:8]
    greet(beside(slabs))
    for copy in send_halo(send_ref, land_ref, send_sem, recv_sem, slabs):
        copy.wait()
    out_ref[...] = jnp.concatenate([land_ref[0, 0:1], land_ref[1, 0:1]], axis=1).astype(jnp.int32)


def exchange(agg_ref, all_ref, send_sem, recv_sem, total):
    part = agg_ref.shape[0] // 9
    me = lax.axis_index("chan")
    peers = others("chan", total)
    copies = []
    for k, (low, high) in enumerate(GROUPS):
        span = slice(low * part, high * part)
        for i, peer in enumerate(peers):
            copies.append(
                pltpu.make_async_remote_copy(
                    src_ref=agg_ref.at[span],
                    dst_ref=all_ref.at[me, span],
                    send_sem=send_sem.at[i, k],
                    recv_sem=recv_sem.at[i, k],
                    device_id=peer,
                    device_id_type=mesh_ids,
                )
            )
    for copy in copies:
        copy.start()
    all_ref[me] = agg_ref[...]

    def component(k):
        for group, (low, high) in enumerate(GROUPS):
            if k == low:
                for copy in copies[group * len(peers) : (group + 1) * len(peers)]:
                    copy.wait_recv()
        span = slice(k * part, (k + 1) * part)
        return jnp.concatenate([all_ref[i, span] for i in range(total)], axis=0)

    return copies, component


class Updates:
    def __init__(self, component, layer, scalar_ref, irrep_ref):
        self.component, self.layer, self.irrep = component, layer, irrep_ref
        chans = irrep_ref.shape[2]
        y = dot(turned(scalar_ref[layer]), component(0))
        self.scalar = silu(y[:chans])
        self.gates = sigmoid(y[chans : 2 * chans]), sigmoid(y[2 * chans :])

    def __getitem__(self, k):
        if k == 0:
            return self.scalar
        kind = 0 if k < 4 else 1
        return self.gates[kind] * dot(self.irrep[self.layer, kind], self.component(k))


def middle_kernel(
    slabs,
    parts,
    block,
    species_ref,
    halo_ref,
    agg_ref,
    embed_ref,
    mix_ref,
    scalar_ref,
    irrep_ref,
    inner_basis_ref,
    outer_basis_ref,
    radial_in_ref,
    radial_mid_ref,
    state_ref,
    scalars_ref,
    table_ref,
    halo_table_ref,
    inner_hidden_ref,
    outer_hidden_ref,
    inner_held_ref,
    outer_held_ref,
    out_sem,
    all_ref,
    send_ref,
    land_ref,
    agg_send,
    agg_recv,
    halo_send,
    halo_recv,
):
    part = mix_ref.shape[2]
    greet(others("chan", parts) + list(beside(slabs)))
    copies, component = exchange(agg_ref, all_ref, agg_send, agg_recv, parts)
    entry = turned(radial_in_ref[1])
    writes = []
    lists = (
        (inner_basis_ref, inner_held_ref, inner_hidden_ref),
        (outer_basis_ref, outer_held_ref, outer_hidden_ref),
    )
    for i, (basis_ref, held_ref, hidden_ref) in enumerate(lists):

        def body(step, carry, basis_ref=basis_ref, held_ref=held_ref):
            span = pl.ds(pl.multiple_of(step * block, block), block)
            held_ref[:, span] = radial(entry, radial_mid_ref[1], basis_ref[:, span])
            return carry

        lax.fori_loop(0, basis_ref.shape[1] // block, body, 0)
        writes.append(pltpu.make_async_copy(held_ref, hidden_ref, out_sem.at[i]))
    onehots = jnp.concatenate(
        [onehot_rows(halo_ref[side : side + 1], table_ref.shape[1]) for side in range(2)], axis=1
    )
    start = initial(embed_ref, species_ref[...])
    outs = Updates(component, 0, scalar_ref, irrep_ref)
    held = halo_ref.shape[1]
    for k in range(9):
        out = outs[k]
        if k == 0:
            for write in writes:
                write.start()
            out += start
            scalars_ref[...] = out
        state_ref[k] = out
        which = 0 if k == 0 else (1 if k < 4 else 2)
        span = slice(k * part, (k + 1) * part)
        mixed = dot(mix_ref[1, which], out.astype(bf16)).astype(bf16)
        table_ref[span] = mixed
        picked = dot(mixed, onehots).astype(bf16)
        for side in range(2):
            send_ref[side, span] = picked[:, side * held : (side + 1) * held]
    for copy in copies:
        copy.wait_send()
    for copy in send_halo(send_ref, land_ref, halo_send, halo_recv, slabs):
        copy.wait()
    for write in writes:
        write.wait()
    for side in range(2):
        halo_table_ref[:, side * held : (side + 1) * held] = land_ref[side]


def energy_kernel(
    slabs,
    parts,
    species_ref,
    count_ref,
    agg_ref,
    scalars_ref,
    scalar_ref,
    readout_ref,
    energy_ref,
    every_ref,
    atom_ref,
    mean_ref,
    all_ref,
    energies_ref,
    agg_send,
    agg_recv,
    energy_send,
    energy_recv,
):
    peers = others("slab", slabs)
    greet(others("chan", parts) + peers)
    copies, component = exchange(agg_ref, all_ref, agg_send, agg_recv, parts)
    chans, atoms = scalars_ref.shape
    lines = lax.broadcasted_iota(jnp.int32, (chans, chans), 0)
    across = lax.broadcasted_iota(jnp.int32, (chans, chans), 1)
    readout = jnp.sum(jnp.where(lines == across, readout_ref[...], 0.0), axis=1, keepdims=True)
    own = jnp.zeros((1, atoms), f32)
    for kind in range(energy_ref.shape[0]):
        own = jnp.where(species_ref[...] == kind, energy_ref[kind], own)
    lanes = lax.broadcasted_iota(jnp.int32, (1, atoms), 1)
    weight = turned(scalar_ref[1])[:chans]
    out = scalars_ref[...] + silu(dot(weight, component(0)))
    total = jnp.sum(out * readout, axis=0, keepdims=True) + own
    total = jnp.where(lanes < count_ref[0], total, 0.0)
    me = lax.axis_index("slab")
    energies_ref[me] = jnp.broadcast_to(
        jnp.sum(total, axis=1, keepdims=True), energies_ref.shape[1:]
    )
    atom_ref[...] = total
    part = agg_ref.shape[0] // 9
    every_ref[:, :part] = all_ref[:, :part]
    sums = [
        pltpu.make_async_remote_copy(
            src_ref=energies_ref.at[me],
            dst_ref=energies_ref.at[me],
            send_sem=energy_send.at[i],
            recv_sem=energy_recv.at[i],
            device_id=peer,
            device_id_type=mesh_ids,
        )
        for i, peer in enumerate(peers)
    ]
    for copy in sums:
        copy.start()
    for k in range(1, 9):
        component(k)
    every_ref[:, part:] = all_ref[:, part:]
    for copy in copies:
        copy.wait_send()
    for copy in sums:
        copy.wait()
    mean_ref[...] = jnp.sum(energies_ref[...], axis=0)[0:1, 0:1] * (1.0 / (atoms * slabs))


def last_kernel(
    every_ref, state_in_ref, scalar_ref, irrep_ref, atom_in_ref, mean_in_ref, state_ref, atom_ref, mean_ref
):
    part = every_ref.shape[1] // 9

    def component(k):
        span = slice(k * part, (k + 1) * part)
        return jnp.concatenate([every_ref[i, span] for i in range(every_ref.shape[0])], axis=0)

    outs = Updates(component, 1, scalar_ref, irrep_ref)
    for k in range(9):
        state_ref[k] = state_in_ref[k] + outs[k]
    atom_ref[...] = atom_in_ref[...]
    mean_ref[...] = mean_in_ref[...]


vmem = pl.BlockSpec(memory_space=pltpu.VMEM)
anywhere = pl.BlockSpec(memory_space=pl.ANY)
smem = pl.BlockSpec(memory_space=pltpu.SMEM)
params = pltpu.CompilerParams(vmem_limit_bytes=56 * 1024 * 1024)


def remote(number):
    return pltpu.CompilerParams(
        vmem_limit_bytes=56 * 1024 * 1024, collective_id=number, has_side_effects=True
    )


def local(
    species,
    atom_count,
    halo_index,
    edge_count,
    inner_edges,
    outer_edges,
    inner_vec,
    outer_vec,
    embed_table,
    radial_in,
    radial_mid,
    radial_out,
    mix_in,
    mix_scalar,
    mix_irrep,
    readout,
    species_energy,
):
    slabs = lax.axis_size("slab")
    parts = lax.axis_size("chan")
    atoms = species.shape[0]
    chans = embed_table.shape[0]
    part = mix_in.shape[2]
    breadth = radial_mid.shape[1]
    basis = radial_in.shape[2]
    paths = radial_out.shape[1]
    halo = halo_index[0]
    held = halo.shape[1]
    rows = 9 * part
    dma = pltpu.SemaphoreType.DMA
    species_row = species[None, :]
    embed = embed_table.T
    scalar = jnp.swapaxes(mix_scalar, 1, 2)
    halo_species = pl.pallas_call(
        functools.partial(species_kernel, slabs),
        out_shape=jax.ShapeDtypeStruct((1, 2 * held), jnp.int32),
        in_specs=[vmem] * 2,
        out_specs=vmem,
        scratch_shapes=[
            pltpu.VMEM((2, 8, held), f32),
            pltpu.VMEM((2, 8, held), f32),
            dma((2,)),
            dma((2,)),
        ],
        compiler_params=remote(0),
        name="halo_species",
    )(species_row, halo)
    block = math.gcd(BLOCK, math.gcd(inner_edges.shape[1], outer_edges.shape[1]))
    inner_total, outer_total = inner_edges.shape[1], outer_edges.shape[1]
    radial_turned = jnp.swapaxes(radial_in, 1, 2)
    agg, inner_basis, outer_basis = pl.pallas_call(
        functools.partial(first_kernel, block),
        out_shape=(
            jax.ShapeDtypeStruct((rows, atoms), bf16),
            jax.ShapeDtypeStruct((basis, inner_total), bf16),
            jax.ShapeDtypeStruct((basis, outer_total), bf16),
        ),
        in_specs=[smem] + [vmem] * 11,
        out_specs=(vmem, vmem, vmem),
        scratch_shapes=[
            pltpu.VMEM((rows, atoms), f32),
            pltpu.VMEM((2, part, atoms), bf16),
            pltpu.VMEM((rows, block), bf16),
            pltpu.VMEM((breadth, basis), bf16),
            pltpu.VMEM((3 * part, breadth), bf16),
        ],
        compiler_params=params,
        name="first_layer",
    )(
        edge_count,
        species_row,
        halo_species,
        inner_edges,
        outer_edges,
        inner_vec,
        outer_vec,
        embed,
        mix_in,
        radial_turned,
        radial_mid,
        radial_out,
    )
    state, scalars, table, halo_table, inner_hidden, outer_hidden = pl.pallas_call(
        functools.partial(
            middle_kernel, slabs, parts, math.gcd(WIDE, math.gcd(inner_total, outer_total))
        ),
        out_shape=(
            jax.ShapeDtypeStruct((9, chans, atoms), f32),
            jax.ShapeDtypeStruct((chans, atoms), f32),
            jax.ShapeDtypeStruct((rows, atoms), bf16),
            jax.ShapeDtypeStruct((rows, 2 * held), bf16),
            jax.ShapeDtypeStruct((breadth, inner_total), bf16),
            jax.ShapeDtypeStruct((breadth, outer_total), bf16),
        ),
        in_specs=[vmem] * 11,
        out_specs=(vmem, vmem, vmem, vmem, anywhere, anywhere),
        scratch_shapes=[
            pltpu.VMEM((breadth, inner_total), bf16),
            pltpu.VMEM((breadth, outer_total), bf16),
            dma((2,)),
            pltpu.VMEM((parts, rows, atoms), bf16),
            pltpu.VMEM((2, rows, held), bf16),
            pltpu.VMEM((2, rows, held), bf16),
            dma((parts - 1, 9)),
            dma((parts - 1, 9)),
            dma((2,)),
            dma((2,)),
        ],
        compiler_params=remote(1),
        name="middle",
    )(
        species_row,
        halo,
        agg,
        embed,
        mix_in,
        scalar,
        mix_irrep,
        inner_basis,
        outer_basis,
        radial_turned,
        radial_mid,
    )
    agg = pl.pallas_call(
        functools.partial(second_kernel, block),
        out_shape=jax.ShapeDtypeStruct((rows, atoms), bf16),
        in_specs=[smem] + [vmem] * 6 + [anywhere] * 2 + [vmem],
        out_specs=vmem,
        scratch_shapes=[
            pltpu.VMEM((rows, atoms), f32),
            pltpu.VMEM((paths * part, block), f32),
            pltpu.VMEM((rows, block), f32),
            pltpu.VMEM((rows, block), bf16),
            pltpu.VMEM((breadth, inner_total), bf16),
            pltpu.VMEM((breadth, outer_total), bf16),
            dma((inner_total // block,)),
            dma((outer_total // block,)),
        ],
        compiler_params=params,
        name="second_layer",
    )(
        edge_count,
        table,
        halo_table,
        inner_edges,
        outer_edges,
        inner_vec,
        outer_vec,
        inner_hidden,
        outer_hidden,
        radial_out,
    )
    every, atom_energy, mean_energy = pl.pallas_call(
        functools.partial(energy_kernel, slabs, parts),
        out_shape=(
            jax.ShapeDtypeStruct((parts, rows, atoms), bf16),
            jax.ShapeDtypeStruct((1, atoms), f32),
            jax.ShapeDtypeStruct((1, 1), f32),
        ),
        in_specs=[vmem, smem] + [vmem] * 4 + [smem],
        out_specs=(vmem, vmem, vmem),
        scratch_shapes=[
            pltpu.VMEM((parts, rows, atoms), bf16),
            pltpu.VMEM((slabs, 8, 128), f32),
            dma((parts - 1, 9)),
            dma((parts - 1, 9)),
            dma((slabs - 1,)),
            dma((slabs - 1,)),
        ],
        compiler_params=remote(2),
        name="energies",
    )(
        species_row,
        atom_count,
        agg,
        scalars,
        scalar,
        readout[None, :],
        species_energy,
    )
    node_state, atom_energy, mean_energy = pl.pallas_call(
        last_kernel,
        out_shape=(
            jax.ShapeDtypeStruct((9, chans, atoms), f32),
            jax.ShapeDtypeStruct((1, atoms), f32),
            jax.ShapeDtypeStruct((1, 1), f32),
        ),
        in_specs=[vmem] * 6,
        out_specs=(vmem, vmem, vmem),
        compiler_params=params,
        name="last",
    )(every, state, scalar, mix_irrep, atom_energy, mean_energy)
    return (node_state, atom_energy[0], mean_energy[0, 0])


def solution(mesh):
    return jax.shard_map(
        local,
        mesh=mesh,
        in_specs=(
            P("slab"),
            P("slab"),
            P("slab", None, None),
            P("slab", None),
            P(None, "slab"),
            P(None, "slab"),
            P(None, "slab"),
            P(None, "slab"),
            P(),
            P(),
            P(),
            P(None, None, "chan", None),
            P(None, None, "chan", None),
            P(),
            P(),
            P(),
            P(),
        ),
        out_specs=(P(None, None, "slab"), P("slab"), P()),
        check_vma=False,
    )
```
